256 devices in a mesh: gx: 4 (over x), gy: 16 (over y, z_hi), gz: 4 (over z_lo, core).
Axes of the slice: x: 4, y: 4, z: 8 (z_hi: 4, z_lo: 2; z = z_hi * 2 + z_lo), core: 2. Of those that a mesh axis runs over, the one named last changes fastest.
Arguments:
- coef: float32 [4, 64, 512, 512], P(None, 'gx', 'gy', 'gz'), may hold values from -6 to 6
- keep: int32 [4, 16, 128, 128], P(None, 'gx', 'gy', 'gz'), may hold values from 1 to 10
- courant: float32 [64, 512, 512], P('gx', 'gy', 'gz'), may hold values from 0.05 to 0.2
- damp: float32 [64, 512, 512], P('gx', 'gy', 'gz'), may hold values from 0 to 0.3
- adj_next: float32 [64, 512, 512], P('gx', 'gy', 'gz'), may hold values from -6 to 6
- adj_now: float32 [64, 512, 512], P('gx', 'gy', 'gz'), may hold values from -6 to 6
- rec_cell: int32 [4, 16, 4, 128], P('gx', 'gy', 'gz'), may hold values from 0 to 65535
- rec_data: float32 [4, 16, 4, 4, 128], P('gx', 'gy', 'gz'), may hold values from -6 to 6
Outputs:
- gradient: float32 [64, 512, 512], P('gx', 'gy', 'gz')
- adjoint_last: float32 [64, 512, 512], P('gx', 'gy', 'gz')
- adjoint_before: float32 [64, 512, 512], P('gx', 'gy', 'gz')
The draws below stay inside these ranges and needn't reach their ends.
Inputs may be any that keep to these rules, and one draw needn't show every extreme that they name: `keep`: A block's coefficient (a, b, c) is kept when a + b + c is below this count. `rec_cell`: A row-major index into the 16 x 32 x 128 cells of the device's own block; indices may repeat.
All inputs are finite; a program needn't handle non-finite values.
Results may differ from the reference program's by a relative error of at most 0.00013.
Values sent between devices are 32-bit elements; how exact they have to be, the bound alone decides.
A program may use at most 64 MiB of HBM per device.

```python
import math
import jax
import jax.numpy as jnp
from jax import lax

CX = 16
CY = 32
CZ = 128
RECS = 128
STEPS = 4
NX = 64
NY = 512
NZ = 512
N_GX = 4
N_GY = 16
N_GZ = 4


def set_ends(array, own_key, low, high):
    spot = [jax.random.randint(jax.random.fold_in(own_key, axis), (), 0, length) for axis, length in enumerate(array.shape)]
    widest = array.shape.index(max(array.shape))
    next_to = spot[:widest] + [(spot[widest] + 1) % array.shape[widest]] + spot[widest + 1:]
    return array.at[tuple(spot)].set(low).at[tuple(next_to)].set(high)


def block_scale(stream_key, dims, split, least, high):
    level = 1.0
    for axis_at, blocks in split:
        steps = jax.random.uniform(jax.random.fold_in(jax.random.fold_in(stream_key, 6), axis_at), (blocks,), jnp.float32, least / len(split), high / len(split))
        level = level * jnp.repeat(jnp.exp(steps), dims[axis_at] // blocks).reshape((-1,) + (1,) * (len(dims) - 1 - axis_at))
    return level


def scatter_about(stream_key, shape, deviation, limit, split=(), kind=jnp.bfloat16):
    entries = deviation * jax.random.normal(stream_key, shape, jnp.float32)
    if split:
        entries = entries * block_scale(stream_key, shape, split, -0.22, 0.18)
    return jnp.clip(entries, -limit, limit).astype(kind)


def setup_inputs(seed: int = 0) -> dict:
    key_of = jax.random.split(jax.random.key(seed), 9)
    coef = scatter_about(key_of[0], (STEPS, NX, NY, NZ), 1.0, 6.0, ((1, 4), (2, 16), (3, 4)), jnp.float32)
    keep = set_ends(jax.random.randint(key_of[1], (STEPS, NX // 4, NY // 4, NZ // 4), 1, 11), jax.random.fold_in(key_of[1], 1), 1, 10).astype(jnp.int32)
    courant = jnp.clip(jnp.exp(math.log(0.2) - 1.3862944 * jax.random.uniform(key_of[2], (NX, NY, NZ), jnp.float32) ** block_scale(key_of[2], (NX, NY, NZ), ((0, 4), (1, 16), (2, 4)), -0.2, 0.2)), 0.05, 0.2)
    damp = jnp.clip(0.3 * jax.random.uniform(key_of[3], (NX, NY, NZ), jnp.float32) ** block_scale(key_of[3], (NX, NY, NZ), ((0, 4), (1, 16), (2, 4)), -0.2, 0.2), 0.0, 0.3)
    adj_next = scatter_about(key_of[4], (NX, NY, NZ), 1.0, 6.0, ((0, 4), (1, 16), (2, 4)), jnp.float32)
    adj_now = scatter_about(key_of[5], (NX, NY, NZ), 1.0, 6.0, ((0, 4), (1, 16), (2, 4)), jnp.float32)
    rec_cell = set_ends(jax.random.randint(key_of[6], (N_GX, N_GY, N_GZ, RECS), 0, CX * CY * CZ), jax.random.fold_in(key_of[6], 1), 0, (CX * CY * CZ) - 1).astype(jnp.int32)
    rec_data = scatter_about(key_of[7], (N_GX, N_GY, N_GZ, STEPS, RECS), 1.0, 6.0, ((0, 4), (1, 16), (2, 4)), jnp.float32)
    return dict(coef=coef, keep=keep, courant=courant, damp=damp, adj_next=adj_next, adj_now=adj_now, rec_cell=rec_cell, rec_data=rec_data)


STAR = (-205.0 / 72.0, 8.0 / 5.0, -1.0 / 5.0, 8.0 / 315.0, -1.0 / 560.0)

def dct_table():
    freq = jnp.arange(4, dtype=jnp.float32)[:, None]
    place = jnp.arange(4, dtype=jnp.float32)[None, :]
    scales = jnp.where(freq == 0.0, 0.5, jnp.sqrt(jnp.float32(0.5)))
    return scales * jnp.cos(jnp.pi * (2.0 * place + 1.0) * freq / 8.0)

def decode(block_coef, block_keep):
    levels = (jnp.arange(NX, dtype=jnp.int32) % 4)[:, None, None] + (jnp.arange(NY, dtype=jnp.int32) % 4)[None, :, None] + (jnp.arange(NZ, dtype=jnp.int32) % 4)[None, None, :]
    spread = jnp.repeat(jnp.repeat(jnp.repeat(block_keep, 4, axis=0), 4, axis=1), 4, axis=2)
    masked = jnp.where(levels < spread, block_coef, 0.0)
    shaped = masked.reshape(NX // 4, 4, NY // 4, 4, NZ // 4, 4)
    table = dct_table()
    out = jnp.einsum('xaybzc,ai,bj,ck->xiyjzk', shaped, table, table, table, precision=lax.Precision.HIGHEST)
    return out.reshape(NX, NY, NZ)

def laplace(field):
    padded = jnp.pad(field, 4)
    size_x, size_y, size_z = field.shape
    total = 3.0 * STAR[0] * field
    for reach in range(1, 5):
        plus_x = padded[4 + reach:4 + reach + size_x, 4:4 + size_y, 4:4 + size_z]
        minus_x = padded[4 - reach:4 - reach + size_x, 4:4 + size_y, 4:4 + size_z]
        plus_y = padded[4:4 + size_x, 4 + reach:4 + reach + size_y, 4:4 + size_z]
        minus_y = padded[4:4 + size_x, 4 - reach:4 - reach + size_y, 4:4 + size_z]
        plus_z = padded[4:4 + size_x, 4:4 + size_y, 4 + reach:4 + reach + size_z]
        minus_z = padded[4:4 + size_x, 4:4 + size_y, 4 - reach:4 - reach + size_z]
        total = total + STAR[reach] * (plus_x + minus_x + plus_y + minus_y + plus_z + minus_z)
    return total

def reference(coef, keep, courant, damp, adj_next, adj_now, rec_cell, rec_data):
    local_x = rec_cell // (CY * CZ)
    local_y = rec_cell // CZ % CY
    local_z = rec_cell % CZ
    global_x = jnp.arange(N_GX, dtype=jnp.int32)[:, None, None, None] * CX + local_x
    global_y = jnp.arange(N_GY, dtype=jnp.int32)[None, :, None, None] * CY + local_y
    global_z = jnp.arange(N_GZ, dtype=jnp.int32)[None, None, :, None] * CZ + local_z
    flat = ((global_x * NY + global_y) * NZ + global_z).reshape(-1).astype(jnp.int32)
    gradient = jnp.zeros((NX, NY, NZ), jnp.float32)
    later = adj_next
    current = adj_now
    for step in range(STEPS):
        forward = decode(coef[step], keep[step])
        gradient = gradient + courant * current * laplace(forward)
        inject = jnp.zeros((NX * NY * NZ,), jnp.float32).at[flat].add(rec_data[:, :, :, step, :].reshape(-1)).reshape(NX, NY, NZ)
        earlier = (2.0 * current - (1.0 - damp) * later + courant * laplace(current) + inject) / (1.0 + damp)
        later = current
        current = earlier
    return (gradient, current, later)
```

```python
import functools

import jax
import jax.numpy as jnp
import numpy as np
from jax import lax
from jax.experimental import pallas as pl
from jax.experimental.pallas import tpu as pltpu
from jax.sharding import PartitionSpec as P

STAR = (-205.0 / 72.0, 8.0 / 5.0, -1.0 / 5.0, 8.0 / 315.0, -1.0 / 560.0)
CX, CY, CZ, STEPS, RECS = 16, 32, 128, 4, 128
ROWS = CX * CY
AXES = ("gx", "gy", "gz")
MESH = pl.DeviceIdType.MESH
F32, BF16 = jnp.float32, jnp.bfloat16


def split_np(table):
    high = table.astype(np.float32).astype(jnp.bfloat16)
    low = (table - high.astype(np.float64)).astype(np.float32).astype(jnp.bfloat16)
    return high, low


def tables():
    freq, place = np.arange(4)[:, None], np.arange(4)[None, :]
    dct = np.where(freq == 0, 0.5, np.sqrt(0.5)) * np.cos(np.pi * (2 * place + 1) * freq / 8)
    along_z = np.kron(np.eye(CZ // 4), dct)
    along_xy = np.kron(dct.T, np.kron(np.eye(CY // 4), dct.T))
    gap = np.abs(np.arange(CZ)[:, None] - np.arange(CZ)[None, :])
    taps = np.select([gap == k for k in range(1, 5)], STAR[1:], 0.0)
    lane = np.arange(CZ)[None, :]
    member = (np.arange(CZ) % 4)[:, None]
    below = np.select([lane + 4 - member == k for k in range(1, 5)], STAR[1:], 0.0)
    above = np.select([128 + member - lane == k for k in range(1, 5)], STAR[1:], 0.0)
    halo = np.concatenate([below, above], axis=0)
    taps_hl = np.concatenate(split_np(taps), axis=1)
    z_hl = np.concatenate(split_np(along_z), axis=1)
    halo_hl = np.concatenate(split_np(halo), axis=1)
    mats = np.stack(
        [np.concatenate([taps_hl, taps_hl]), np.concatenate([z_hl, z_hl]), halo_hl]
    )
    decode_xy = np.concatenate(split_np(along_xy), axis=1)
    spread_z = np.kron(np.eye(CZ // 4), np.ones((1, 4))).astype(jnp.bfloat16)
    spread_y = np.kron(np.eye(STEPS * CX // 4), np.kron(np.eye(CY // 4), np.ones((4, 1))))
    return mats, decode_xy, spread_z, spread_y.astype(jnp.bfloat16)


def split(value):
    high = value.astype(BF16)
    low = (value - high.astype(F32)).astype(BF16)
    return high, low


def dot(a, b):
    return lax.dot_general(a, b, (((1,), (0,)), ((), ())), preferred_element_type=F32)


def halves(value):
    return value[:, :CZ] + value[:, CZ:]


def kernel(
    coef, keep, cour, damp, nxt, now, cell, data, mats, dxy, spz, spy,
    grad_o, last_o, before_o,
    F, cin, kin, cour_v, damp_v, next_v, cell_v, data_v, mats_v, dxy_v, spz_v, spy_v,
    wa, wb, we, inj, thr, Z, E, G, last_v, XH, YP, YH, ZP, ZH,
    load_sem, store_sem, send_sem, recv_sem,
):
    me = [lax.axis_index(axis) for axis in AXES]
    size = [lax.axis_size(axis) for axis in AXES]
    has = [(me[d] > 0, me[d] < size[d] - 1) for d in range(3)]
    other = [({AXES[d]: me[d] - 1}, {AXES[d]: me[d] + 1}) for d in range(3)]

    loads = [
        pltpu.make_async_copy(src, dst, load_sem.at[n])
        for n, (src, dst) in enumerate(
            [
                (now, F.at[0, pl.ds(4, CX), pl.ds(8, CY)]),
                (mats, mats_v), (keep, kin), (spz, spz_v), (spy, spy_v), (dxy, dxy_v),
                (coef, cin), (damp, damp_v), (cour, cour_v), (nxt, next_v),
                (cell, cell_v), (data, data_v),
            ]
        )
    ]
    for load in loads:
        load.start()

    barrier = pltpu.get_barrier_semaphore()
    for d in range(3):
        for side in range(2):
            @pl.when(has[d][side])
            def _():
                pl.semaphore_signal(
                    barrier, inc=1, device_id=other[d][side], device_id_type=MESH
                )

    def clear(f, carry):
        F[f, 0:4] = jnp.zeros((4, 48, CZ), F32)
        F[f, 20:24] = jnp.zeros((4, 48, CZ), F32)
        F[f, 4:20, 0:8] = jnp.zeros((CX, 8, CZ), F32)
        F[f, 4:20, 40:48] = jnp.zeros((CX, 8, CZ), F32)
        for side in range(2):
            YH[f, side, 0:8] = jnp.zeros((8, CZ), F32)
            YH[f, side, 72:80] = jnp.zeros((8, CZ), F32)

            @pl.when(jnp.logical_not(has[0][side]))
            def _():
                XH[f, side] = jnp.zeros((4, CY, CZ), F32)

            @pl.when(jnp.logical_not(has[1][side]))
            def _():
                YH[f, side, 8:72] = jnp.zeros((64, CZ), F32)

            @pl.when(jnp.logical_not(has[2][side]))
            def _():
                ZH[f, side] = jnp.zeros((16, CZ), F32)

        return carry

    lax.fori_loop(0, 8, clear, 0)

    lane = lax.broadcasted_iota(jnp.int32, (8, CZ), 1)
    sub = lax.broadcasted_iota(jnp.int32, (8, CZ), 0)
    near_low = [None] + [jnp.where(sub < k, STAR[k], 0.0).astype(F32) for k in range(1, 5)]
    near_high = [None] + [jnp.where(sub >= 8 - k, STAR[k], 0.0).astype(F32) for k in range(1, 5)]

    def face(f, d, side):
        if d == 0:
            src = F.at[f, pl.ds(4 if side == 0 else CX, 4), pl.ds(8, CY)]
            dst = XH.at[f, 1 - side]
        elif d == 1:
            src, dst = YP.at[f, side], YH.at[f, 1 - side, pl.ds(8, 64)]
        else:
            src, dst = ZP.at[f, side], ZH.at[f, 1 - side]
        return pltpu.make_async_remote_copy(
            src_ref=src,
            dst_ref=dst,
            send_sem=send_sem.at[f, 2 * d + side],
            recv_sem=recv_sem.at[f, 2 * d + 1 - side],
            device_id=other[d][side],
            device_id_type=MESH,
        )

    def pack(f):
        def pack_y(p, carry):
            for side, row in ((0, 8), (1, 36)):
                two = [F[f, 4 + 2 * p + q, row : row + 4, :] for q in range(2)]
                YP[f, side, pl.ds(pl.multiple_of(8 * p, 8), 8), :] = jnp.concatenate(two, axis=0)
            return carry

        lax.fori_loop(0, 8, pack_y, 0, unroll=True)

        def pack_z(q, kept):
            kept = list(kept)
            for tile in range(4):
                i = 4 * q + tile
                here = lane // 4 == i
                for half in range(2):
                    value = F[f, 4 + 8 * half + q, 8 + 8 * tile : 16 + 8 * tile, :]
                    low = pltpu.roll(value, 4 * i, 1)
                    high = pltpu.roll(value, (4 * i + 4) % CZ, 1)
                    kept[half] = jnp.where(here, low, kept[half])
                    kept[2 + half] = jnp.where(here, high, kept[2 + half])
            return tuple(kept)

        zero = jnp.zeros((8, CZ), F32)
        kept = lax.fori_loop(0, 8, pack_z, (zero,) * 4, unroll=True)
        for side in range(2):
            for half in range(2):
                ZP[f, side, 8 * half : 8 * half + 8, :] = kept[2 * side + half]

    def send(f):
        for d in (1, 0, 2):
            for side in range(2):
                @pl.when(has[d][side])
                def _():
                    face(f, d, side).start()

    def arrive(f):
        for d in (0, 2, 1):
            for side in range(2):
                @pl.when(has[d][side])
                def _():
                    face(f, d, 1 - side).wait_recv()

    def own_z(f):
        value = F[f, 4:20, 8:40, :].reshape(ROWS, CZ)
        return halves(dot(jnp.concatenate(split(value), axis=1), mats_v[0]))

    def far_z(f):
        group = lax.broadcasted_iota(jnp.int32, (1, 32, 8, CZ), 1)
        lanes = lax.broadcasted_iota(jnp.int32, (1, 32, 8, CZ), 3)
        here = lanes // 4 == group
        highs, lows = [], []
        for side in range(2):
            value = ZH[f, side]
            high = value.astype(BF16).astype(F32)
            for part, out in ((high, highs), (value - high, lows)):
                wide = jnp.where(here, part.reshape(2, 1, 8, CZ), 0.0)
                out.append(wide.reshape(ROWS, CZ).astype(BF16))
        total = dot(jnp.concatenate(highs, axis=1), mats_v[2])
        total = total + dot(jnp.concatenate(lows, axis=1), mats_v[2])
        return halves(total)

    def add_far(f):
        for i in range(4):
            low = sum(STAR[k] * XH[f, 0, 4 + i - k] for k in range(i + 1, 5))
            Z[i] = Z[i] + low
            high = sum(STAR[4 + m - i] * XH[f, 1, m] for m in range(i + 1))
            Z[12 + i] = Z[12 + i] + high
        for x in range(CX):
            low = sum(near_low[k] * YH[f, 0, 12 + 4 * x - k : 20 + 4 * x - k] for k in range(1, 5))
            high = sum(near_high[k] * YH[f, 1, 4 * x + k : 4 * x + k + 8] for k in range(1, 5))
            Z[x, 0:8] = Z[x, 0:8] + low
            Z[x, 24:32] = Z[x, 24:32] + high

    def own_star(f, x):
        total = (3.0 * STAR[0]) * F[f, 4 + x, 8:40, :] + Z[x]
        for k in range(1, 5):
            pairs = F[f, 4 + x + k, 8:40, :] + F[f, 4 + x - k, 8:40, :]
            pairs = pairs + F[f, 4 + x, 8 + k : 40 + k, :] + F[f, 4 + x, 8 - k : 40 - k, :]
            total = total + STAR[k] * pairs
        return total

    def adjoint_own(s):
        Z[...] = own_z(s).reshape(CX, CY, CZ)

        def step(x, carry):
            later = next_v[x] if s == 0 else F[s - 1, 4 + x, 8:40, :]
            E[x] = (
                wa[x] * F[s, 4 + x, 8:40, :]
                - wb[x] * later
                + we[x] * own_star(s, x)
                + inj[s, x]
            )
            return carry

        lax.fori_loop(0, CX, step, 0, unroll=2)

    def adjoint_far(s):
        arrive(s)
        Z[...] = far_z(s).reshape(CX, CY, CZ)
        add_far(s)

        def step(x, carry):
            value = E[x] + we[x] * Z[x]
            if s == STEPS - 1:
                last_v[x] = value
            else:
                F[s + 1, 4 + x, 8:40, :] = value
            return carry

        lax.fori_loop(0, CX, step, 0, unroll=4)

    def decode(s):
        level = (
            lax.broadcasted_iota(jnp.int32, (CY, CZ), 0) % 4
            + lax.broadcasted_iota(jnp.int32, (CY, CZ), 1) % 4
        ).astype(F32)
        masked = [
            jnp.where(level + float(x % 4) < thr[s, x // 4], cin[s, x], 0.0) for x in range(CX)
        ]
        value = jnp.concatenate(masked, axis=0)
        along_z = halves(dot(jnp.concatenate(split(value), axis=1), mats_v[1]))
        for g in range(CX // 4):
            both = jnp.concatenate(split(along_z[CZ * g : CZ * g + CZ]), axis=1)
            out = halves(dot(dxy_v[...], jnp.concatenate([both, both], axis=0)))
            F[4 + s, 4 + 4 * g : 8 + 4 * g, 8:40, :] = out.reshape(4, CY, CZ)

    def gradient(s):
        f = 4 + s
        arrive(f)
        Z[...] = (own_z(f) + far_z(f)).reshape(CX, CY, CZ)
        add_far(f)

        def step(x, carry):
            value = cour_v[x] * F[s, 4 + x, 8:40, :] * own_star(f, x)
            G[x] = value if s == 0 else G[x] + value
            return carry

        lax.fori_loop(0, CX, step, 0, unroll=2)

    loads[0].wait()
    pack(0)
    peers = sum(there.astype(jnp.int32) for pair in has for there in pair)
    pl.semaphore_wait(barrier, peers)
    send(0)

    for load in loads[1:7]:
        load.wait()
    levels = kin[...].reshape(STEPS * (CX // 4) * (CY // 4), CZ // 4).astype(F32).astype(BF16)
    wide = dot(levels, spz_v[...]).astype(BF16)
    thr[...] = dot(spy_v[...], wide).reshape(STEPS, CX // 4, CY, CZ)
    for s in range(2):
        decode(s)
        pack(4 + s)
        send(4 + s)

    for load in loads[7:]:
        load.wait()

    def weights(x, carry):
        over = 1.0 / (1.0 + damp_v[x])
        wa[x] = 2.0 * over
        wb[x] = (1.0 - damp_v[x]) * over
        we[x] = cour_v[x] * over
        return carry

    lax.fori_loop(0, CX, weights, 0, unroll=2)

    row = lax.broadcasted_iota(jnp.int32, (ROWS, RECS), 0)
    rows_hot = jnp.where(row == cell_v[...] // CZ, 1.0, 0.0).astype(BF16)
    rows_hot = jnp.concatenate([rows_hot, rows_hot], axis=1)
    at_lane = lax.broadcasted_iota(jnp.int32, (CZ, RECS), 0) == cell_v[...] % CZ
    for s in range(STEPS):
        lanes_hot = jnp.where(at_lane, data_v[s : s + 1, :], 0.0)
        lanes_hot = jnp.concatenate(split(lanes_hot), axis=1)
        spread = lax.dot_general(
            rows_hot, lanes_hot, (((1,), (1,)), ((), ())), preferred_element_type=F32
        )
        inj[s] = spread.reshape(CX, CY, CZ) * (0.5 * wa[...])

    stores = [
        pltpu.make_async_copy(G, grad_o, store_sem.at[0]),
        pltpu.make_async_copy(last_v, last_o, store_sem.at[1]),
        pltpu.make_async_copy(
            F.at[STEPS - 1, pl.ds(4, CX), pl.ds(8, CY)], before_o, store_sem.at[2]
        ),
    ]
    adjoint_own(0)
    for s in range(STEPS):
        adjoint_far(s)
        if s < STEPS - 1:
            pack(s + 1)
            send(s + 1)
            if s == STEPS - 2:
                stores[2].start()
            if s < 2:
                decode(2 + s)
                pack(6 + s)
                send(6 + s)
            adjoint_own(s + 1)
            gradient(s)
            if s == STEPS - 2:
                gradient(s + 1)
                stores[0].start()
    stores[1].start()
    for f in range(8):
        for d in range(3):
            for side in range(2):
                @pl.when(has[d][side])
                def _():
                    face(f, d, side).wait_send()
    for store in stores:
        store.wait()


def local(coef, keep, courant, damp, adj_next, adj_now, rec_cell, rec_data):
    shape = (CX, CY, CZ)
    block = jax.ShapeDtypeStruct(shape, F32)
    mats, dxy, spz, spy = tables()
    vmem = pltpu.VMEM
    scratch = [
        vmem((8, 24, 48, CZ), F32),
        vmem((STEPS,) + shape, F32),
        vmem((STEPS, CX // 4, CY // 4, CZ // 4), jnp.int32),
        vmem(shape, F32), vmem(shape, F32), vmem(shape, F32),
        vmem((1, RECS), jnp.int32), vmem((STEPS, RECS), F32),
        vmem(mats.shape, BF16), vmem(dxy.shape, BF16), vmem(spz.shape, BF16), vmem(spy.shape, BF16),
        vmem(shape, F32), vmem(shape, F32), vmem(shape, F32),
        vmem((STEPS,) + shape, F32),
        vmem((STEPS, CX // 4, CY, CZ), F32),
        vmem(shape, F32), vmem(shape, F32), vmem(shape, F32), vmem(shape, F32),
        vmem((8, 2, 4, CY, CZ), F32),
        vmem((8, 2, 64, CZ), F32), vmem((8, 2, 80, CZ), F32),
        vmem((8, 2, 16, CZ), F32), vmem((8, 2, 16, CZ), F32),
        pltpu.SemaphoreType.DMA((12,)), pltpu.SemaphoreType.DMA((3,)),
        pltpu.SemaphoreType.DMA((8, 6)), pltpu.SemaphoreType.DMA((8, 6)),
    ]
    anywhere = pl.BlockSpec(memory_space=pl.ANY)
    return pl.pallas_call(
        kernel,
        out_shape=(block, block, block),
        in_specs=[pl.BlockSpec(memory_space=pltpu.HBM)] * 12,
        out_specs=(anywhere,) * 3,
        scratch_shapes=scratch,
        compiler_params=pltpu.CompilerParams(
            collective_id=0, has_side_effects=True, vmem_limit_bytes=48 * 1024 * 1024
        ),
        name="adjoint_window",
    )(
        coef, keep, courant, damp, adj_next, adj_now,
        rec_cell.reshape(1, RECS), rec_data.reshape(STEPS, RECS),
        jnp.asarray(mats), jnp.asarray(dxy), jnp.asarray(spz), jnp.asarray(spy),
    )


def solution(mesh):
    field = P("gx", "gy", "gz")
    in_specs = (
        P(None, "gx", "gy", "gz"), P(None, "gx", "gy", "gz"),
        field, field, field, field,
        P("gx", "gy", "gz", None), P("gx", "gy", "gz", None, None),
    )
    return jax.shard_map(
        local, mesh=mesh, in_specs=in_specs, out_specs=(field,) * 3, check_vma=False
    )
```

```python
import functools

import jax
import jax.numpy as jnp
import numpy as np
from jax import lax
from jax.experimental import pallas as pl
from jax.experimental.pallas import tpu as pltpu
from jax.sharding import PartitionSpec as P

STAR = (-205.0 / 72.0, 8.0 / 5.0, -1.0 / 5.0, 8.0 / 315.0, -1.0 / 560.0)
CX, CY, CZ, STEPS, RECS = 16, 32, 128, 4, 128
ROWS = CX * CY
AXES = ("gx", "gy", "gz")
MESH = pl.DeviceIdType.MESH
F32, BF16 = jnp.float32, jnp.bfloat16


def split_np(table):
    high = table.astype(np.float32).astype(jnp.bfloat16)
    low = (table - high.astype(np.float64)).astype(np.float32).astype(jnp.bfloat16)
    return high, low


def tables():
    freq, place = np.arange(4)[:, None], np.arange(4)[None, :]
    dct = np.where(freq == 0, 0.5, np.sqrt(0.5)) * np.cos(np.pi * (2 * place + 1) * freq / 8)
    along_z = np.kron(np.eye(CZ // 4), dct)
    along_xy = np.kron(dct.T, np.kron(np.eye(CY // 4), dct.T))
    gap = np.abs(np.arange(CZ)[:, None] - np.arange(CZ)[None, :])
    taps = np.select([gap == k for k in range(1, 5)], STAR[1:], 0.0)
    lane = np.arange(CZ)[None, :]
    member = (np.arange(CZ) % 4)[:, None]
    below = np.select([lane + 4 - member == k for k in range(1, 5)], STAR[1:], 0.0)
    above = np.select([128 + member - lane == k for k in range(1, 5)], STAR[1:], 0.0)
    halo = np.concatenate([below, above], axis=0)
    taps_hl = np.concatenate(split_np(taps), axis=1)
    z_hl = np.concatenate(split_np(along_z), axis=1)
    halo_hl = np.concatenate(split_np(halo), axis=1)
    mats = np.stack(
        [np.concatenate([taps_hl, taps_hl]), np.concatenate([z_hl, z_hl]), halo_hl]
    )
    decode_xy = np.concatenate(split_np(along_xy), axis=1)
    spread_z = np.kron(np.eye(CZ // 4), np.ones((1, 4))).astype(jnp.bfloat16)
    spread_y = np.kron(np.eye(STEPS * CX // 4), np.kron(np.eye(CY // 4), np.ones((4, 1))))
    return mats, decode_xy, spread_z, spread_y.astype(jnp.bfloat16)


def split(value):
    high = value.astype(BF16)
    low = (value - high.astype(F32)).astype(BF16)
    return high, low


def dot(a, b):
    return lax.dot_general(a, b, (((1,), (0,)), ((), ())), preferred_element_type=F32)


def halves(value):
    return value[:, :CZ] + value[:, CZ:]


def kernel(
    coef, keep, cour, damp, nxt, now, cell, data, mats, dxy, spz, spy,
    grad_o, last_o, before_o,
    F, cin, kin, cour_v, damp_v, next_v, cell_v, data_v, mats_v, dxy_v, spz_v, spy_v,
    wa, wb, we, inj, thr, Z, E, XH, YP, YH, ZP, ZH,
    load_sem, send_sem, recv_sem,
):
    me = [lax.axis_index(axis) for axis in AXES]
    size = [lax.axis_size(axis) for axis in AXES]
    has = [(me[d] > 0, me[d] < size[d] - 1) for d in range(3)]
    other = [({AXES[d]: me[d] - 1}, {AXES[d]: me[d] + 1}) for d in range(3)]

    loads = [
        pltpu.make_async_copy(src, dst, load_sem.at[n])
        for n, (src, dst) in enumerate(
            [
                (now, F.at[0, pl.ds(4, CX), pl.ds(8, CY)]),
                (mats, mats_v), (keep, kin), (spz, spz_v), (spy, spy_v), (dxy, dxy_v),
                (coef, cin), (damp, damp_v), (cour, cour_v), (nxt, next_v),
                (cell, cell_v), (data, data_v),
            ]
        )
    ]
    for load in loads:
        load.start()

    barrier = pltpu.get_barrier_semaphore()
    for d in range(3):
        for side in range(2):
            @pl.when(has[d][side])
            def _():
                pl.semaphore_signal(
                    barrier, inc=1, device_id=other[d][side], device_id_type=MESH
                )

    def clear(f, carry):
        F[f, 0:4] = jnp.zeros((4, 48, CZ), F32)
        F[f, 20:24] = jnp.zeros((4, 48, CZ), F32)
        F[f, 4:20, 0:8] = jnp.zeros((CX, 8, CZ), F32)
        F[f, 4:20, 40:48] = jnp.zeros((CX, 8, CZ), F32)
        for side in range(2):
            YH[f, side, 0:8] = jnp.zeros((8, CZ), F32)
            YH[f, side, 72:80] = jnp.zeros((8, CZ), F32)

            @pl.when(jnp.logical_not(has[0][side]))
            def _():
                XH[f, side] = jnp.zeros((4, CY, CZ), F32)

            @pl.when(jnp.logical_not(has[1][side]))
            def _():
                YH[f, side, 8:72] = jnp.zeros((64, CZ), F32)

            @pl.when(jnp.logical_not(has[2][side]))
            def _():
                ZH[f, side] = jnp.zeros((16, CZ), F32)

        return carry

    lax.fori_loop(0, 8, clear, 0)

    lane = lax.broadcasted_iota(jnp.int32, (8, CZ), 1)
    sub = lax.broadcasted_iota(jnp.int32, (8, CZ), 0)
    near_low = [None] + [jnp.where(sub < k, STAR[k], 0.0).astype(F32) for k in range(1, 5)]
    near_high = [None] + [jnp.where(sub >= 8 - k, STAR[k], 0.0).astype(F32) for k in range(1, 5)]

    def face(f, d, side):
        if d == 0:
            src = F.at[f, pl.ds(4 if side == 0 else CX, 4), pl.ds(8, CY)]
            dst = XH.at[f, 1 - side]
        elif d == 1:
            src, dst = YP.at[f, side], YH.at[f, 1 - side, pl.ds(8, 64)]
        else:
            src, dst = ZP.at[f, side], ZH.at[f, 1 - side]
        return pltpu.make_async_remote_copy(
            src_ref=src,
            dst_ref=dst,
            send_sem=send_sem.at[f, 2 * d + side],
            recv_sem=recv_sem.at[f, 2 * d + 1 - side],
            device_id=other[d][side],
            device_id_type=MESH,
        )

    def pack(f):
        def pack_y(p, carry):
            for side, row in ((0, 8), (1, 36)):
                two = [F[f, 4 + 2 * p + q, row : row + 4, :] for q in range(2)]
                YP[f, side, pl.ds(pl.multiple_of(8 * p, 8), 8), :] = jnp.concatenate(two, axis=0)
            return carry

        lax.fori_loop(0, 8, pack_y, 0, unroll=True)

        def pack_z(q, kept):
            kept = list(kept)
            for tile in range(4):
                i = 4 * q + tile
                here = lane // 4 == i
                for half in range(2):
                    value = F[f, 4 + 8 * half + q, 8 + 8 * tile : 16 + 8 * tile, :]
                    low = pltpu.roll(value, 4 * i, 1)
                    high = pltpu.roll(value, (4 * i + 4) % CZ, 1)
                    kept[half] = jnp.where(here, low, kept[half])
                    kept[2 + half] = jnp.where(here, high, kept[2 + half])
            return tuple(kept)

        zero = jnp.zeros((8, CZ), F32)
        kept = lax.fori_loop(0, 8, pack_z, (zero,) * 4, unroll=True)
        for side in range(2):
            for half in range(2):
                ZP[f, side, 8 * half : 8 * half + 8, :] = kept[2 * side + half]

    def send(f):
        for d in (1, 0, 2):
            for side in range(2):
                @pl.when(has[d][side])
                def _():
                    face(f, d, side).start()

    def arrive(f):
        for d in (0, 2, 1):
            for side in range(2):
                @pl.when(has[d][side])
                def _():
                    face(f, d, 1 - side).wait_recv()

    def own_z(f):
        value = F[f, 4:20, 8:40, :].reshape(ROWS, CZ)
        return halves(dot(jnp.concatenate(split(value), axis=1), mats_v[0]))

    def far_z(f):
        group = lax.broadcasted_iota(jnp.int32, (1, 32, 8, CZ), 1)
        lanes = lax.broadcasted_iota(jnp.int32, (1, 32, 8, CZ), 3)
        here = lanes // 4 == group
        highs, lows = [], []
        for side in range(2):
            value = ZH[f, side]
            high = value.astype(BF16).astype(F32)
            for part, out in ((high, highs), (value - high, lows)):
                wide = jnp.where(here, part.reshape(2, 1, 8, CZ), 0.0)
                out.append(wide.reshape(ROWS, CZ).astype(BF16))
        total = dot(jnp.concatenate(highs, axis=1), mats_v[2])
        total = total + dot(jnp.concatenate(lows, axis=1), mats_v[2])
        return halves(total)

    def add_far(f):
        for i in range(4):
            low = sum(STAR[k] * XH[f, 0, 4 + i - k] for k in range(i + 1, 5))
            Z[i] = Z[i] + low
            high = sum(STAR[4 + m - i] * XH[f, 1, m] for m in range(i + 1))
            Z[12 + i] = Z[12 + i] + high
        for x in range(CX):
            low = sum(near_low[k] * YH[f, 0, 12 + 4 * x - k : 20 + 4 * x - k] for k in range(1, 5))
            high = sum(near_high[k] * YH[f, 1, 4 * x + k : 4 * x + k + 8] for k in range(1, 5))
            Z[x, 0:8] = Z[x, 0:8] + low
            Z[x, 24:32] = Z[x, 24:32] + high

    def own_star(f, x):
        total = (3.0 * STAR[0]) * F[f, 4 + x, 8:40, :] + Z[x]
        for k in range(1, 5):
            pairs = F[f, 4 + x + k, 8:40, :] + F[f, 4 + x - k, 8:40, :]
            pairs = pairs + F[f, 4 + x, 8 + k : 40 + k, :] + F[f, 4 + x, 8 - k : 40 - k, :]
            total = total + STAR[k] * pairs
        return total

    def adjoint_own(s):
        Z[...] = own_z(s).reshape(CX, CY, CZ)

        def step(x, carry):
            later = next_v[x] if s == 0 else F[s - 1, 4 + x, 8:40, :]
            E[x] = (
                wa[x] * F[s, 4 + x, 8:40, :]
                - wb[x] * later
                + we[x] * own_star(s, x)
                + inj[s, x]
            )
            return carry

        lax.fori_loop(0, CX, step, 0, unroll=2)

    def adjoint_far(s):
        arrive(s)
        Z[...] = far_z(s).reshape(CX, CY, CZ)
        add_far(s)

        def step(x, carry):
            value = E[x] + we[x] * Z[x]
            if s == STEPS - 1:
                last_o[x] = value
            else:
                F[s + 1, 4 + x, 8:40, :] = value
            if s == STEPS - 2:
                before_o[x] = value
            return carry

        lax.fori_loop(0, CX, step, 0, unroll=4)

    def decode(s):
        level = (
            lax.broadcasted_iota(jnp.int32, (CY, CZ), 0) % 4
            + lax.broadcasted_iota(jnp.int32, (CY, CZ), 1) % 4
        ).astype(F32)
        masked = [
            jnp.where(level + float(x % 4) < thr[s, x // 4], cin[s, x], 0.0) for x in range(CX)
        ]
        value = jnp.concatenate(masked, axis=0)
        along_z = halves(dot(jnp.concatenate(split(value), axis=1), mats_v[1]))
        for g in range(CX // 4):
            both = jnp.concatenate(split(along_z[CZ * g : CZ * g + CZ]), axis=1)
            out = halves(dot(dxy_v[...], jnp.concatenate([both, both], axis=0)))
            F[4 + s, 4 + 4 * g : 8 + 4 * g, 8:40, :] = out.reshape(4, CY, CZ)

    def gradient(s):
        f = 4 + s
        arrive(f)
        Z[...] = (own_z(f) + far_z(f)).reshape(CX, CY, CZ)
        add_far(f)

        def step(x, carry):
            value = cour_v[x] * F[s, 4 + x, 8:40, :] * own_star(f, x)
            grad_o[x] = value if s == 0 else grad_o[x] + value
            return carry

        lax.fori_loop(0, CX, step, 0, unroll=2)

    loads[0].wait()
    pack(0)
    peers = sum(there.astype(jnp.int32) for pair in has for there in pair)
    pl.semaphore_wait(barrier, peers)
    send(0)

    for load in loads[1:7]:
        load.wait()
    levels = kin[...].reshape(STEPS * (CX // 4) * (CY // 4), CZ // 4).astype(F32).astype(BF16)
    wide = dot(levels, spz_v[...]).astype(BF16)
    thr[...] = dot(spy_v[...], wide).reshape(STEPS, CX // 4, CY, CZ)
    for s in range(2):
        decode(s)
        pack(4 + s)
        send(4 + s)

    for load in loads[7:]:
        load.wait()

    def weights(x, carry):
        over = 1.0 / (1.0 + damp_v[x])
        wa[x] = 2.0 * over
        wb[x] = (1.0 - damp_v[x]) * over
        we[x] = cour_v[x] * over
        return carry

    lax.fori_loop(0, CX, weights, 0, unroll=2)

    row = lax.broadcasted_iota(jnp.int32, (ROWS, RECS), 0)
    rows_hot = jnp.where(row == cell_v[...] // CZ, 1.0, 0.0).astype(BF16)
    rows_hot = jnp.concatenate([rows_hot, rows_hot], axis=1)
    at_lane = lax.broadcasted_iota(jnp.int32, (CZ, RECS), 0) == cell_v[...] % CZ
    for s in range(STEPS):
        lanes_hot = jnp.where(at_lane, data_v[s : s + 1, :], 0.0)
        lanes_hot = jnp.concatenate(split(lanes_hot), axis=1)
        spread = lax.dot_general(
            rows_hot, lanes_hot, (((1,), (1,)), ((), ())), preferred_element_type=F32
        )
        inj[s] = spread.reshape(CX, CY, CZ) * (0.5 * wa[...])

    adjoint_own(0)
    for s in range(STEPS):
        adjoint_far(s)
        if s < STEPS - 1:
            pack(s + 1)
            send(s + 1)
            if s < 2:
                decode(2 + s)
                pack(6 + s)
                send(6 + s)
            adjoint_own(s + 1)
            gradient(s)
            if s == STEPS - 2:
                gradient(s + 1)
    for f in range(8):
        for d in range(3):
            for side in range(2):
                @pl.when(has[d][side])
                def _():
                    face(f, d, side).wait_send()


def put_out(grad_v, last_v, before_v, grad_o, last_o, before_o, sem):
    pairs = ((grad_v, grad_o), (last_v, last_o), (before_v, before_o))
    copies = [pltpu.make_async_copy(v, o, sem.at[n]) for n, (v, o) in enumerate(pairs)]
    for copy in copies:
        copy.start()
    for copy in copies:
        copy.wait()


def local(coef, keep, courant, damp, adj_next, adj_now, rec_cell, rec_data):
    shape = (CX, CY, CZ)
    block = jax.ShapeDtypeStruct(shape, F32)
    mats, dxy, spz, spy = tables()
    vmem = pltpu.VMEM
    scratch = [
        vmem((8, 24, 48, CZ), F32),
        vmem((STEPS,) + shape, F32),
        vmem((STEPS, CX // 4, CY // 4, CZ // 4), jnp.int32),
        vmem(shape, F32), vmem(shape, F32), vmem(shape, F32),
        vmem((1, RECS), jnp.int32), vmem((STEPS, RECS), F32),
        vmem(mats.shape, BF16), vmem(dxy.shape, BF16), vmem(spz.shape, BF16), vmem(spy.shape, BF16),
        vmem(shape, F32), vmem(shape, F32), vmem(shape, F32),
        vmem((STEPS,) + shape, F32),
        vmem((STEPS, CX // 4, CY, CZ), F32),
        vmem(shape, F32), vmem(shape, F32),
        vmem((8, 2, 4, CY, CZ), F32),
        vmem((8, 2, 64, CZ), F32), vmem((8, 2, 80, CZ), F32),
        vmem((8, 2, 16, CZ), F32), vmem((8, 2, 16, CZ), F32),
        pltpu.SemaphoreType.DMA((12,)),
        pltpu.SemaphoreType.DMA((8, 6)), pltpu.SemaphoreType.DMA((8, 6)),
    ]
    vmem_spec = pl.BlockSpec(memory_space=pltpu.VMEM)
    hbm_spec = pl.BlockSpec(memory_space=pltpu.HBM)
    results = pl.pallas_call(
        kernel,
        out_shape=(vmem(shape, F32),) * 3,
        in_specs=[hbm_spec] * 12,
        out_specs=(vmem_spec,) * 3,
        scratch_shapes=scratch,
        compiler_params=pltpu.CompilerParams(
            collective_id=0, has_side_effects=True, vmem_limit_bytes=67043328 - 3 * 4 * CX * CY * CZ
        ),
        name="adjoint_window",
    )(
        coef, keep, courant, damp, adj_next, adj_now,
        rec_cell.reshape(1, RECS), rec_data.reshape(STEPS, RECS),
        jnp.asarray(mats), jnp.asarray(dxy), jnp.asarray(spz), jnp.asarray(spy),
    )
    return pl.pallas_call(
        put_out,
        out_shape=(block,) * 3,
        in_specs=[pl.BlockSpec(memory_space=pl.ANY)] * 3,
        out_specs=(hbm_spec,) * 3,
        scratch_shapes=[pltpu.SemaphoreType.DMA((3,))],
        compiler_params=pltpu.CompilerParams(vmem_limit_bytes=1024 * 1024),
        name="put_out",
    )(*results)


def solution(mesh):
    field = P("gx", "gy", "gz")
    in_specs = (
        P(None, "gx", "gy", "gz"), P(None, "gx", "gy", "gz"),
        field, field, field, field,
        P("gx", "gy", "gz", None), P("gx", "gy", "gz", None, None),
    )
    return jax.shard_map(
        local, mesh=mesh, in_specs=in_specs, out_specs=(field,) * 3, check_vma=False
    )
```

```python
import functools

import jax
import jax.numpy as jnp
import numpy as np
from jax import lax
from jax.experimental import pallas as pl
from jax.experimental.pallas import tpu as pltpu
from jax.sharding import PartitionSpec as P

STAR = (-205.0 / 72.0, 8.0 / 5.0, -1.0 / 5.0, 8.0 / 315.0, -1.0 / 560.0)
CX, CY, CZ, STEPS, RECS = 16, 32, 128, 4, 128
ROWS = CX * CY
PIECES = 2
PART = 64 // PIECES
AXES = ("gx", "gy", "gz")
MESH = pl.DeviceIdType.MESH
F32, BF16 = jnp.float32, jnp.bfloat16


def split_np(table):
    high = table.astype(np.float32).astype(jnp.bfloat16)
    low = (table - high.astype(np.float64)).astype(np.float32).astype(jnp.bfloat16)
    return high, low


def tables():
    freq, place = np.arange(4)[:, None], np.arange(4)[None, :]
    dct = np.where(freq == 0, 0.5, np.sqrt(0.5)) * np.cos(np.pi * (2 * place + 1) * freq / 8)
    along_z = np.kron(np.eye(CZ // 4), dct)
    along_xy = np.kron(dct.T, np.kron(np.eye(CY // 4), dct.T))
    gap = np.abs(np.arange(CZ)[:, None] - np.arange(CZ)[None, :])
    taps = np.select([gap == k for k in range(1, 5)], STAR[1:], 0.0)
    taps_hl = np.concatenate(split_np(taps), axis=1)
    z_hl = np.concatenate(split_np(along_z), axis=1)
    mats = np.stack(
        [np.concatenate([taps_hl, taps_hl]), np.concatenate([z_hl, z_hl])]
    )
    decode_xy = np.concatenate(split_np(along_xy), axis=1)
    spread_z = np.kron(np.eye(CZ // 4), np.ones((1, 4))).astype(jnp.bfloat16)
    spread_y = np.kron(np.eye(STEPS * CX // 4), np.kron(np.eye(CY // 4), np.ones((4, 1))))
    return mats, decode_xy, spread_z, spread_y.astype(jnp.bfloat16)


def split(value):
    high = value.astype(BF16)
    low = (value - high.astype(F32)).astype(BF16)
    return high, low


def dot(a, b):
    return lax.dot_general(a, b, (((1,), (0,)), ((), ())), preferred_element_type=F32)


def halves(value):
    return value[:, :CZ] + value[:, CZ:]


def kernel(
    coef, keep, cour, damp, nxt, now, cell, data, mats, dxy, spz, spy,
    grad_o, last_o, before_o,
    F, cin, kin, cour_v, damp_v, next_v, cell_v, data_v, mats_v, dxy_v, spz_v, spy_v,
    wa, wb, we, inj, thr, Z, XH, YP, YH, ZP, ZH,
    load_sem, send_sem, recv_sem,
):
    me = [lax.axis_index(axis) for axis in AXES]
    size = [lax.axis_size(axis) for axis in AXES]
    has = [(me[d] > 0, me[d] < size[d] - 1) for d in range(3)]
    other = [({AXES[d]: me[d] - 1}, {AXES[d]: me[d] + 1}) for d in range(3)]

    loads = [
        pltpu.make_async_copy(src, dst, load_sem.at[n])
        for n, (src, dst) in enumerate(
            [
                (now, F.at[0, pl.ds(4, CX), pl.ds(8, CY)]),
                (mats, mats_v), (keep, kin), (spz, spz_v), (spy, spy_v), (dxy, dxy_v),
                (coef, cin), (damp, damp_v), (cour, cour_v), (nxt, next_v),
                (cell, cell_v), (data, data_v),
            ]
        )
    ]
    for load in loads:
        load.start()

    barrier = pltpu.get_barrier_semaphore()
    for d in range(3):
        for side in range(2):
            @pl.when(has[d][side])
            def _():
                pl.semaphore_signal(
                    barrier, inc=1, device_id=other[d][side], device_id_type=MESH
                )

    def clear(f, carry):
        F[f, 0:4] = jnp.zeros((4, 48, CZ), F32)
        F[f, 20:24] = jnp.zeros((4, 48, CZ), F32)
        F[f, 4:20, 0:8] = jnp.zeros((CX, 8, CZ), F32)
        F[f, 4:20, 40:48] = jnp.zeros((CX, 8, CZ), F32)
        for side in range(2):
            for n in range(PIECES):
                YH[f, side, n, 0:8] = jnp.zeros((8, CZ), F32)
                YH[f, side, n, 8 + PART : 16 + PART] = jnp.zeros((8, CZ), F32)

            @pl.when(jnp.logical_not(has[0][side]))
            def _():
                XH[f, side] = jnp.zeros((4, CY, CZ), F32)

            @pl.when(jnp.logical_not(has[1][side]))
            def _():
                YH[f, side, :, 8 : 8 + PART] = jnp.zeros((PIECES, PART, CZ), F32)

            @pl.when(jnp.logical_not(has[2][side]))
            def _():
                ZH[f, side] = jnp.zeros((16, CZ), F32)

        return carry

    lax.fori_loop(0, 8, clear, 0)

    lane = lax.broadcasted_iota(jnp.int32, (8, CZ), 1)
    sub = lax.broadcasted_iota(jnp.int32, (8, CZ), 0)
    near_low = [None] + [jnp.where(sub < k, STAR[k], 0.0).astype(F32) for k in range(1, 5)]
    near_high = [None] + [jnp.where(sub >= 8 - k, STAR[k], 0.0).astype(F32) for k in range(1, 5)]

    def faces(f, d, side, some=slice(None)):
        if d == 0:
            start = 4 if side == 0 else CX
            rows = ((8, 16), (0, 8), (24, 8)) if f < STEPS else ((0, CY),)
            pairs = [
                (
                    F.at[f, pl.ds(start, 4), pl.ds(8 + row, count)],
                    XH.at[f, 1 - side, slice(None), pl.ds(row, count)],
                )
                for row, count in rows
            ]
        elif d == 1:
            pairs = [
                (YP.at[f, side, pl.ds(PART * n, PART)], YH.at[f, 1 - side, n, pl.ds(8, PART)])
                for n in range(PIECES)
            ]
        else:
            pairs = [(ZP.at[f, side], ZH.at[f, 1 - side])]
        return [
            pltpu.make_async_remote_copy(
                src_ref=src,
                dst_ref=dst,
                send_sem=send_sem.at[f, 2 * d + side, n],
                recv_sem=recv_sem.at[f, 2 * d + 1 - side, n],
                device_id=other[d][side],
                device_id_type=MESH,
            )
            for n, (src, dst) in list(enumerate(pairs))[some]
        ]

    def each_side(d, act):
        for side in range(2):
            @pl.when(has[d][side])
            def _():
                act(side)

    def send(f, d, some=slice(None)):
        each_side(d, lambda side: [copy.start() for copy in faces(f, d, side, some)])

    def arrive(f, d, some=slice(None)):
        each_side(d, lambda side: [copy.wait_recv() for copy in faces(f, d, 1 - side, some)])

    def drain(f, d):
        each_side(d, lambda side: [copy.wait_send() for copy in faces(f, d, side)])

    def pack_rows(f):
        def pack_y(p, carry):
            for side, row in ((0, 8), (1, 36)):
                two = [F[f, 4 + 2 * p + q, row : row + 4, :] for q in range(2)]
                YP[f, side, pl.ds(pl.multiple_of(8 * p, 8), 8), :] = jnp.concatenate(two, axis=0)
            return carry

        lax.fori_loop(0, 8, pack_y, 0, unroll=True)

    def pack_lanes(f):
        def pack_z(q, kept):
            kept = list(kept)
            for tile in range(4):
                i = 4 * q + tile
                here = lane // 4 == i
                for half in range(2):
                    value = F[f, 4 + 8 * half + q, 8 + 8 * tile : 16 + 8 * tile, :]
                    low = pltpu.roll(value, 4 * i, 1)
                    high = pltpu.roll(value, (4 * i + 4) % CZ, 1)
                    kept[half] = jnp.where(here, low, kept[half])
                    kept[2 + half] = jnp.where(here, high, kept[2 + half])
            return tuple(kept)

        zero = jnp.zeros((8, CZ), F32)
        kept = lax.fori_loop(0, 8, pack_z, (zero,) * 4, unroll=True)
        for side in range(2):
            for half in range(2):
                ZP[f, side, 8 * half : 8 * half + 8, :] = kept[2 * side + half]

    def own_z(f):
        value = F[f, 4:20, 8:40, :].reshape(ROWS, CZ)
        return halves(dot(jnp.concatenate(split(value), axis=1), mats_v[0]))

    def far_z(f):
        member = lane % 4
        out = []
        for half in range(2):
            low = ZH[f, 0, 8 * half : 8 * half + 8, :]
            high = ZH[f, 1, 8 * half : 8 * half + 8, :]
            low_sum = STAR[4] * low
            high_sum = STAR[4] * high
            for k in range(1, 4):
                gap = 4 - k
                low_sum = low_sum + jnp.where(
                    member < k, STAR[k] * pltpu.roll(low, CZ - gap, 1), 0.0
                )
                high_sum = high_sum + jnp.where(
                    member >= gap, STAR[k] * pltpu.roll(high, gap, 1), 0.0
                )
            out.append((low_sum, high_sum))
        return out

    def add_z(f, target, scale):
        packed = far_z(f)
        for v in range(64):
            half, i = divmod(v, 32)
            low = pltpu.roll(packed[half][0], (CZ - 4 * i) % CZ, 1)
            high = pltpu.roll(packed[half][1], (252 - 4 * i) % CZ, 1)
            value = jnp.where(lane < 4, low, jnp.where(lane >= CZ - 4, high, 0.0))
            x, row = v // 4, 8 * (v % 4)
            if scale is not None:
                value = scale[x, row : row + 8] * value
            target[x, row : row + 8] = target[x, row : row + 8] + value

    def add_x(f, target, scale):
        for i in range(4):
            low = sum(STAR[k] * XH[f, 0, 4 + i - k] for k in range(i + 1, 5))
            high = sum(STAR[4 + m - i] * XH[f, 1, m] for m in range(i + 1))
            if scale is not None:
                low, high = scale[i] * low, scale[12 + i] * high
            target[i] = target[i] + low
            target[12 + i] = target[12 + i] + high

    def near_y(f, x):
        n, at = divmod(4 * x, PART)
        low = sum(near_low[k] * YH[f, 0, n, 12 + at - k : 20 + at - k] for k in range(1, 5))
        high = sum(near_high[k] * YH[f, 1, n, at + k : at + k + 8] for k in range(1, 5))
        return low, high

    def own_star(f, x):
        total = (3.0 * STAR[0]) * F[f, 4 + x, 8:40, :] + Z[x]
        for k in range(1, 5):
            pairs = F[f, 4 + x + k, 8:40, :] + F[f, 4 + x - k, 8:40, :]
            pairs = pairs + F[f, 4 + x, 8 + k : 40 + k, :] + F[f, 4 + x, 8 - k : 40 - k, :]
            total = total + STAR[k] * pairs
        return total

    def target_of(s):
        return last_o if s == STEPS - 1 else F.at[s + 1, pl.ds(4, CX), pl.ds(8, CY)]

    def adjoint_own(s):
        Z[...] = own_z(s).reshape(CX, CY, CZ)
        target = target_of(s)

        def step(x, carry):
            later = next_v[x] if s == 0 else F[s - 1, 4 + x, 8:40, :]
            current = F[s, 4 + x, 8:40, :]
            target[x] = wa[x] * current - wb[x] * later + we[x] * own_star(s, x) + inj[s, x]
            if s == STEPS - 1:
                before_o[x] = current
            return carry

        lax.fori_loop(0, CX, step, 0, unroll=2)

    def adjoint_far(s):
        target = target_of(s)
        sends = s < STEPS - 1
        arrive(s, 2)
        add_z(s, target, we)
        arrive(s, 0)
        add_x(s, target, we)
        if sends:
            send(s + 1, 0, slice(0, 1))
        for piece in range(PIECES):
            arrive(s, 1, slice(piece, piece + 1))
            for p in range(8 * piece // PIECES, 8 * (piece + 1) // PIECES):
                lows, highs = [], []
                for x in (2 * p, 2 * p + 1):
                    low, high = near_y(s, x)
                    low = target[x, 0:8] + we[x, 0:8] * low
                    high = target[x, 24:32] + we[x, 24:32] * high
                    lows.append(low[0:4])
                    highs.append(high[4:8])
                    target[x, 0:8] = low
                    target[x, 24:32] = high
                if sends:
                    YP[s + 1, 0, 8 * p : 8 * p + 8] = jnp.concatenate(lows, axis=0)
                    YP[s + 1, 1, 8 * p : 8 * p + 8] = jnp.concatenate(highs, axis=0)
            if sends:
                send(s + 1, 1, slice(piece, piece + 1))
        if sends:
            send(s + 1, 0, slice(1, 3))
            pack_lanes(s + 1)
            send(s + 1, 2)

    def decode(s):
        level = (
            lax.broadcasted_iota(jnp.int32, (CY, CZ), 0) % 4
            + lax.broadcasted_iota(jnp.int32, (CY, CZ), 1) % 4
        ).astype(F32)
        masked = [
            jnp.where(level + float(x % 4) < thr[s, x // 4], cin[s, x], 0.0) for x in range(CX)
        ]
        value = jnp.concatenate(masked, axis=0)
        along_z = halves(dot(jnp.concatenate(split(value), axis=1), mats_v[1]))
        for g in range(CX // 4):
            both = jnp.concatenate(split(along_z[CZ * g : CZ * g + CZ]), axis=1)
            out = halves(dot(dxy_v[...], jnp.concatenate([both, both], axis=0)))
            F[4 + s, 4 + 4 * g : 8 + 4 * g, 8:40, :] = out.reshape(4, CY, CZ)

    def gradient(s):
        f = 4 + s
        Z[...] = own_z(f).reshape(CX, CY, CZ)
        arrive(f, 2)
        add_z(f, Z, None)
        arrive(f, 0)
        add_x(f, Z, None)
        arrive(f, 1)
        for x in range(CX):
            low, high = near_y(f, x)
            Z[x, 0:8] = Z[x, 0:8] + low
            Z[x, 24:32] = Z[x, 24:32] + high

        def step(x, carry):
            value = cour_v[x] * F[s, 4 + x, 8:40, :] * own_star(f, x)
            grad_o[x] = value if s == 0 else grad_o[x] + value
            return carry

        lax.fori_loop(0, CX, step, 0, unroll=2)

    def send_forward(s):
        decode(s)
        pack_rows(4 + s)
        pack_lanes(4 + s)
        for d in (1, 0, 2):
            send(4 + s, d)

    loads[0].wait()
    pack_rows(0)
    pack_lanes(0)
    peers = sum(there.astype(jnp.int32) for pair in has for there in pair)
    pl.semaphore_wait(barrier, peers)
    for d in (1, 0, 2):
        send(0, d)

    for load in loads[1:7]:
        load.wait()
    levels = kin[...].reshape(STEPS * (CX // 4) * (CY // 4), CZ // 4).astype(F32).astype(BF16)
    wide = dot(levels, spz_v[...]).astype(BF16)
    thr[...] = dot(spy_v[...], wide).reshape(STEPS, CX // 4, CY, CZ)
    for s in range(2):
        send_forward(s)

    for load in loads[7:]:
        load.wait()

    def weights(x, carry):
        over = 1.0 / (1.0 + damp_v[x])
        wa[x] = 2.0 * over
        wb[x] = (1.0 - damp_v[x]) * over
        we[x] = cour_v[x] * over
        return carry

    lax.fori_loop(0, CX, weights, 0, unroll=2)

    row = lax.broadcasted_iota(jnp.int32, (ROWS, RECS), 0)
    rows_hot = jnp.where(row == cell_v[...] // CZ, 1.0, 0.0).astype(BF16)
    rows_hot = jnp.concatenate([rows_hot, rows_hot], axis=1)
    at_lane = lax.broadcasted_iota(jnp.int32, (CZ, RECS), 0) == cell_v[...] % CZ
    for s in range(STEPS):
        lanes_hot = jnp.where(at_lane, data_v[s : s + 1, :], 0.0)
        lanes_hot = jnp.concatenate(split(lanes_hot), axis=1)
        spread = lax.dot_general(
            rows_hot, lanes_hot, (((1,), (1,)), ((), ())), preferred_element_type=F32
        )
        inj[s] = spread.reshape(CX, CY, CZ) * (0.5 * wa[...])

    adjoint_own(0)
    for s in range(STEPS):
        adjoint_far(s)
        if s < STEPS - 1:
            if s < 2:
                send_forward(2 + s)
            adjoint_own(s + 1)
            gradient(s)
            if s == STEPS - 2:
                gradient(s + 1)
    for f in range(2 * STEPS):
        for d in range(3):
            drain(f, d)


def put_out(grad_v, last_v, before_v, grad_o, last_o, before_o, sem):
    pairs = ((grad_v, grad_o), (last_v, last_o), (before_v, before_o))
    copies = [pltpu.make_async_copy(v, o, sem.at[n]) for n, (v, o) in enumerate(pairs)]
    for copy in copies:
        copy.start()
    for copy in copies:
        copy.wait()


def local(coef, keep, courant, damp, adj_next, adj_now, rec_cell, rec_data):
    shape = (CX, CY, CZ)
    block = jax.ShapeDtypeStruct(shape, F32)
    mats, dxy, spz, spy = tables()
    vmem = pltpu.VMEM
    scratch = [
        vmem((8, 24, 48, CZ), F32),
        vmem((STEPS,) + shape, F32),
        vmem((STEPS, CX // 4, CY // 4, CZ // 4), jnp.int32),
        vmem(shape, F32), vmem(shape, F32), vmem(shape, F32),
        vmem((1, RECS), jnp.int32), vmem((STEPS, RECS), F32),
        vmem(mats.shape, BF16), vmem(dxy.shape, BF16), vmem(spz.shape, BF16), vmem(spy.shape, BF16),
        vmem(shape, F32), vmem(shape, F32), vmem(shape, F32),
        vmem((STEPS,) + shape, F32),
        vmem((STEPS, CX // 4, CY, CZ), F32),
        vmem(shape, F32),
        vmem((8, 2, 4, CY, CZ), F32),
        vmem((8, 2, 64, CZ), F32), vmem((8, 2, PIECES, 16 + PART, CZ), F32),
        vmem((8, 2, 16, CZ), F32), vmem((8, 2, 16, CZ), F32),
        pltpu.SemaphoreType.DMA((12,)),
        pltpu.SemaphoreType.DMA((8, 6, 3)), pltpu.SemaphoreType.DMA((8, 6, 3)),
    ]
    vmem_spec = pl.BlockSpec(memory_space=pltpu.VMEM)
    hbm_spec = pl.BlockSpec(memory_space=pltpu.HBM)
    results = pl.pallas_call(
        kernel,
        out_shape=(vmem(shape, F32),) * 3,
        in_specs=[hbm_spec] * 12,
        out_specs=(vmem_spec,) * 3,
        scratch_shapes=scratch,
        compiler_params=pltpu.CompilerParams(
            collective_id=0, has_side_effects=True, vmem_limit_bytes=67043328 - 3 * 4 * CX * CY * CZ
        ),
        name="adjoint_window",
    )(
        coef, keep, courant, damp, adj_next, adj_now,
        rec_cell.reshape(1, RECS), rec_data.reshape(STEPS, RECS),
        jnp.asarray(mats), jnp.asarray(dxy), jnp.asarray(spz), jnp.asarray(spy),
    )
    return pl.pallas_call(
        put_out,
        out_shape=(block,) * 3,
        in_specs=[pl.BlockSpec(memory_space=pl.ANY)] * 3,
        out_specs=(hbm_spec,) * 3,
        scratch_shapes=[pltpu.SemaphoreType.DMA((3,))],
        compiler_params=pltpu.CompilerParams(vmem_limit_bytes=1024 * 1024),
        name="put_out",
    )(*results)


def solution(mesh):
    field = P("gx", "gy", "gz")
    in_specs = (
        P(None, "gx", "gy", "gz"), P(None, "gx", "gy", "gz"),
        field, field, field, field,
        P("gx", "gy", "gz", None), P("gx", "gy", "gz", None, None),
    )
    return jax.shard_map(
        local, mesh=mesh, in_specs=in_specs, out_specs=(field,) * 3, check_vma=False
    )
```

```python
import functools

import jax
import jax.numpy as jnp
import numpy as np
from jax import lax
from jax.experimental import pallas as pl
from jax.experimental.pallas import tpu as pltpu
from jax.sharding import PartitionSpec as P

STAR = (-205.0 / 72.0, 8.0 / 5.0, -1.0 / 5.0, 8.0 / 315.0, -1.0 / 560.0)
CX, CY, CZ, STEPS, RECS = 16, 32, 128, 4, 128
ROWS = CX * CY
PIECES = 4
PART = 64 // PIECES
AXES = ("gx", "gy", "gz")
MESH = pl.DeviceIdType.MESH
F32, BF16 = jnp.float32, jnp.bfloat16


def split_np(table):
    high = table.astype(np.float32).astype(jnp.bfloat16)
    low = (table - high.astype(np.float64)).astype(np.float32).astype(jnp.bfloat16)
    return high, low


def tables():
    freq, place = np.arange(4)[:, None], np.arange(4)[None, :]
    dct = np.where(freq == 0, 0.5, np.sqrt(0.5)) * np.cos(np.pi * (2 * place + 1) * freq / 8)
    along_z = np.kron(np.eye(CZ // 4), dct)
    along_xy = np.kron(dct.T, np.kron(np.eye(CY // 4), dct.T))
    gap = np.abs(np.arange(CZ)[:, None] - np.arange(CZ)[None, :])
    taps = np.select([gap == k for k in range(1, 5)], STAR[1:], 0.0)
    taps_hl = np.concatenate(split_np(taps), axis=1)
    z_hl = np.concatenate(split_np(along_z), axis=1)
    decode_xy = np.concatenate(split_np(along_xy), axis=1)
    spread_z = np.kron(np.eye(CZ // 4), np.ones((1, 4)))
    spread_y = np.kron(np.eye(STEPS * CX // 4), np.kron(np.eye(CY // 4), np.ones((4, 1))))
    spread = np.concatenate([spread_z, spread_y]).astype(jnp.bfloat16)
    spread = np.pad(spread, ((0, 0), (0, CZ)))
    return np.concatenate([taps_hl, taps_hl, z_hl, z_hl, decode_xy, spread])


def split(value):
    high = value.astype(BF16)
    low = (value - high.astype(F32)).astype(BF16)
    return high, low


def dot(a, b):
    return lax.dot_general(a, b, (((1,), (0,)), ((), ())), preferred_element_type=F32)


def halves(value):
    return value[:, :CZ] + value[:, CZ:]


def kernel(
    coef, keep, cour, damp, nxt, now, cell, data, ops,
    grad_o, last_o, before_o,
    F, cin, kin, edge_v, trio, cell_v, data_v, ops_v,
    wa, wb, we, inj, thr, Z, XH, YP, YH, ZP, ZH,
    load_sem, send_sem, step_sem, forward_sem,
):
    me = [lax.axis_index(axis) for axis in AXES]
    size = [lax.axis_size(axis) for axis in AXES]
    has = [(me[d] > 0, me[d] < size[d] - 1) for d in range(3)]
    other = [({AXES[d]: me[d] - 1}, {AXES[d]: me[d] + 1}) for d in range(3)]

    barrier = pltpu.get_barrier_semaphore()
    for d in range(3):
        for side in range(2):
            @pl.when(has[d][side])
            def _():
                pl.semaphore_signal(
                    barrier, inc=1, device_id=other[d][side], device_id_type=MESH
                )

    def load(n, src, dst):
        return pltpu.make_async_copy(src, dst, load_sem.at[n])

    edges = [load(n, now.at[:, pl.ds(24 * n, 8)], edge_v.at[n]) for n in range(2)]
    first = load(2, now, F.at[0, pl.ds(4, CX), pl.ds(8, CY)])
    tables_in = [load(3, ops, ops_v), load(4, keep, kin), load(5, coef, cin)]
    points_in = [load(7, cell, cell_v), load(8, data, data_v)]
    fields_in = [load(6, src, trio.at[n]) for n, src in enumerate((cour, damp, nxt))]
    cour_v, damp_v, next_v = (trio.at[n] for n in range(3))
    for copy in edges + [first]:
        copy.start()

    def clear(f, carry):
        F[f, 0:4] = jnp.zeros((4, 48, CZ), F32)
        F[f, 20:24] = jnp.zeros((4, 48, CZ), F32)
        F[f, 4:20, 0:8] = jnp.zeros((CX, 8, CZ), F32)
        F[f, 4:20, 40:48] = jnp.zeros((CX, 8, CZ), F32)
        for side in range(2):
            for n in range(PIECES):
                YH[f, side, n, 0:8] = jnp.zeros((8, CZ), F32)
                YH[f, side, n, 8 + PART : 16 + PART] = jnp.zeros((8, CZ), F32)

            @pl.when(jnp.logical_not(has[0][side]))
            def _():
                XH[f, side] = jnp.zeros((4, CY, CZ), F32)

            @pl.when(jnp.logical_not(has[1][side]))
            def _():
                YH[f, side, :, 8 : 8 + PART] = jnp.zeros((PIECES, PART, CZ), F32)

            @pl.when(jnp.logical_not(has[2][side]))
            def _():
                ZH[f, side] = jnp.zeros((16, CZ), F32)

        return carry

    lax.fori_loop(0, 8, clear, 0)

    lane = lax.broadcasted_iota(jnp.int32, (8, CZ), 1)
    sub = lax.broadcasted_iota(jnp.int32, (8, CZ), 0)
    near_low = [None] + [jnp.where(sub < k, STAR[k], 0.0).astype(F32) for k in range(1, 5)]
    near_high = [None] + [jnp.where(sub >= 8 - k, STAR[k], 0.0).astype(F32) for k in range(1, 5)]

    def faces(f, d, side, some=slice(None)):
        if d == 0:
            start = 4 if side == 0 else CX
            rows = ((8, 16), (0, 8), (24, 8)) if f < STEPS else ((0, CY),)
            pairs = [
                (
                    F.at[f, pl.ds(start, 4), pl.ds(8 + row, count)],
                    XH.at[f, 1 - side, slice(None), pl.ds(row, count)],
                )
                for row, count in rows
            ]
        elif d == 1:
            pairs = [
                (YP.at[f, side, pl.ds(PART * n, PART)], YH.at[f, 1 - side, n, pl.ds(8, PART)])
                for n in range(PIECES)
            ]
        else:
            pairs = [(ZP.at[f, side], ZH.at[f, 1 - side])]
        return [
            copy_to(f, d, side, n if d == 1 else 0, src, dst)
            for n, (src, dst) in list(enumerate(pairs))[some]
        ]

    def copy_to(f, d, side, n, src, dst):
        if f < STEPS:
            landed = step_sem.at[f % 2, 1 - side, (0, 2 + n, 1)[d]]
        else:
            landed = forward_sem.at[f - STEPS, d, 1 - side]
        return pltpu.make_async_remote_copy(
            src_ref=src,
            dst_ref=dst,
            send_sem=send_sem.at[d, side],
            recv_sem=landed,
            device_id=other[d][side],
            device_id_type=MESH,
        )

    def whole(f, d, side):
        from_ref, to_ref = ((XH, XH), (YP, YP), (ZP, ZH))[d]
        return copy_to(f, d, side, 0, from_ref.at[f, side], to_ref.at[f, 1 - side])

    def each_side(d, act):
        for side in range(2):
            @pl.when(has[d][side])
            def _():
                act(side)

    def send(f, d, some=slice(None)):
        each_side(d, lambda side: [copy.start() for copy in faces(f, d, side, some)])

    def arrive(f, d, piece=None):
        if piece is None:
            each_side(d, lambda side: whole(f, d, 1 - side).wait_recv())
        else:
            some = slice(piece, piece + 1)
            each_side(d, lambda side: [copy.wait_recv() for copy in faces(f, d, 1 - side, some)])

    def drain(d):
        every = (XH, YP, ZP)[d]
        each_side(
            d, lambda side: copy_to(0, d, side, 0, every.at[:, side], every.at[:, side]).wait_send()
        )

    def pack_rows(f):
        def pack_y(p, carry):
            for side, row in ((0, 8), (1, 36)):
                two = [F[f, 4 + 2 * p + q, row : row + 4, :] for q in range(2)]
                YP[f, side, pl.ds(pl.multiple_of(8 * p, 8), 8), :] = jnp.concatenate(two, axis=0)
            return carry

        lax.fori_loop(0, 8, pack_y, 0, unroll=True)

    def pack_lanes(f):
        def pack_z(q, kept):
            kept = list(kept)
            for tile in range(4):
                i = 4 * q + tile
                here = lane // 4 == i
                for half in range(2):
                    value = F[f, 4 + 8 * half + q, 8 + 8 * tile : 16 + 8 * tile, :]
                    low = pltpu.roll(value, 4 * i, 1)
                    high = pltpu.roll(value, (4 * i + 4) % CZ, 1)
                    kept[half] = jnp.where(here, low, kept[half])
                    kept[2 + half] = jnp.where(here, high, kept[2 + half])
            return tuple(kept)

        zero = jnp.zeros((8, CZ), F32)
        kept = lax.fori_loop(0, 8, pack_z, (zero,) * 4, unroll=True)
        for side in range(2):
            for half in range(2):
                ZP[f, side, 8 * half : 8 * half + 8, :] = kept[2 * side + half]

    def own_z(f):
        value = F[f, 4:20, 8:40, :].reshape(ROWS, CZ)
        return halves(dot(jnp.concatenate(split(value), axis=1), ops_v[0:256]))

    def far_z(f):
        member = lane % 4
        out = []
        for half in range(2):
            low = ZH[f, 0, 8 * half : 8 * half + 8, :]
            high = ZH[f, 1, 8 * half : 8 * half + 8, :]
            low_sum = STAR[4] * low
            high_sum = STAR[4] * high
            for k in range(1, 4):
                gap = 4 - k
                low_sum = low_sum + jnp.where(
                    member < k, STAR[k] * pltpu.roll(low, CZ - gap, 1), 0.0
                )
                high_sum = high_sum + jnp.where(
                    member >= gap, STAR[k] * pltpu.roll(high, gap, 1), 0.0
                )
            out.append((low_sum, high_sum))
        return out

    def add_z(f, target, scale):
        packed = far_z(f)
        for v in range(64):
            half, i = divmod(v, 32)
            low = pltpu.roll(packed[half][0], (CZ - 4 * i) % CZ, 1)
            high = pltpu.roll(packed[half][1], (252 - 4 * i) % CZ, 1)
            value = jnp.where(lane < 4, low, jnp.where(lane >= CZ - 4, high, 0.0))
            x, row = v // 4, 8 * (v % 4)
            if scale is not None:
                value = scale[x, row : row + 8] * value
            target[x, row : row + 8] = target[x, row : row + 8] + value

    def add_x(f, target, scale):
        for i in range(4):
            low = sum(STAR[k] * XH[f, 0, 4 + i - k] for k in range(i + 1, 5))
            high = sum(STAR[4 + m - i] * XH[f, 1, m] for m in range(i + 1))
            if scale is not None:
                low, high = scale[i] * low, scale[12 + i] * high
            target[i] = target[i] + low
            target[12 + i] = target[12 + i] + high

    def near_y(f, x):
        n, at = divmod(4 * x, PART)
        low = sum(near_low[k] * YH[f, 0, n, 12 + at - k : 20 + at - k] for k in range(1, 5))
        high = sum(near_high[k] * YH[f, 1, n, at + k : at + k + 8] for k in range(1, 5))
        return low, high

    def own_star(f, x):
        total = (3.0 * STAR[0]) * F[f, 4 + x, 8:40, :] + Z[x]
        for k in range(1, 5):
            pairs = F[f, 4 + x + k, 8:40, :] + F[f, 4 + x - k, 8:40, :]
            pairs = pairs + F[f, 4 + x, 8 + k : 40 + k, :] + F[f, 4 + x, 8 - k : 40 - k, :]
            total = total + STAR[k] * pairs
        return total

    def target_of(s):
        return last_o if s == STEPS - 1 else F.at[s + 1, pl.ds(4, CX), pl.ds(8, CY)]

    def adjoint_own(s):
        Z[...] = own_z(s).reshape(CX, CY, CZ)
        target = target_of(s)

        def step(x, carry):
            later = next_v[x] if s == 0 else F[s - 1, 4 + x, 8:40, :]
            current = F[s, 4 + x, 8:40, :]
            target[x] = wa[x] * current - wb[x] * later + we[x] * own_star(s, x) + inj[s, x]
            if s == STEPS - 1:
                before_o[x] = current
            return carry

        lax.fori_loop(0, CX, step, 0, unroll=2)

    def adjoint_far(s):
        target = target_of(s)
        sends = s < STEPS - 1
        arrive(s, 2)
        add_z(s, target, we)
        arrive(s, 0)
        add_x(s, target, we)
        if sends:
            send(s + 1, 0, slice(0, 1))
        for piece in range(PIECES):
            arrive(s, 1, piece)
            for p in range(8 * piece // PIECES, 8 * (piece + 1) // PIECES):
                lows, highs = [], []
                for x in (2 * p, 2 * p + 1):
                    low, high = near_y(s, x)
                    low = target[x, 0:8] + we[x, 0:8] * low
                    high = target[x, 24:32] + we[x, 24:32] * high
                    lows.append(low[0:4])
                    highs.append(high[4:8])
                    target[x, 0:8] = low
                    target[x, 24:32] = high
                if sends:
                    YP[s + 1, 0, 8 * p : 8 * p + 8] = jnp.concatenate(lows, axis=0)
                    YP[s + 1, 1, 8 * p : 8 * p + 8] = jnp.concatenate(highs, axis=0)
            if sends:
                send(s + 1, 1, slice(piece, piece + 1))
        if sends:
            send(s + 1, 0, slice(1, 3))
            pack_lanes(s + 1)
            send(s + 1, 2)

    def decode(s):
        level = (
            lax.broadcasted_iota(jnp.int32, (CY, CZ), 0) % 4
            + lax.broadcasted_iota(jnp.int32, (CY, CZ), 1) % 4
        ).astype(F32)
        masked = [
            jnp.where(level + float(x % 4) < thr[s, x // 4], cin[s, x], 0.0) for x in range(CX)
        ]
        value = jnp.concatenate(masked, axis=0)
        along_z = halves(dot(jnp.concatenate(split(value), axis=1), ops_v[256:512]))
        for g in range(CX // 4):
            both = jnp.concatenate(split(along_z[CZ * g : CZ * g + CZ]), axis=1)
            out = halves(dot(ops_v[512:640], jnp.concatenate([both, both], axis=0)))
            F[4 + s, 4 + 4 * g : 8 + 4 * g, 8:40, :] = out.reshape(4, CY, CZ)

    def gradient(s):
        f = 4 + s
        Z[...] = own_z(f).reshape(CX, CY, CZ)
        arrive(f, 2)
        add_z(f, Z, None)
        arrive(f, 0)
        add_x(f, Z, None)
        arrive(f, 1)
        for x in range(CX):
            low, high = near_y(f, x)
            Z[x, 0:8] = Z[x, 0:8] + low
            Z[x, 24:32] = Z[x, 24:32] + high

        def step(x, carry):
            value = cour_v[x] * F[s, 4 + x, 8:40, :] * own_star(f, x)
            grad_o[x] = value if s == 0 else grad_o[x] + value
            return carry

        lax.fori_loop(0, CX, step, 0, unroll=2)

    def send_forward(s):
        decode(s)
        pack_rows(4 + s)
        pack_lanes(4 + s)
        for d in (1, 0, 2):
            send(4 + s, d)

    for copy in edges:
        copy.wait()
    for copy in tables_in + fields_in + points_in:
        copy.start()
    for p in range(8):
        for side in range(2):
            two = [edge_v[side, 2 * p + q, 4 * side : 4 * side + 4, :] for q in range(2)]
            YP[0, side, 8 * p : 8 * p + 8, :] = jnp.concatenate(two, axis=0)
    peers = sum(there.astype(jnp.int32) for pair in has for there in pair)
    pl.semaphore_wait(barrier, peers)
    send(0, 1)
    first.wait()
    send(0, 0)
    pack_lanes(0)
    send(0, 2)

    for copy in tables_in:
        copy.wait()
    levels = kin[...].reshape(STEPS * (CX // 4) * (CY // 4), CZ // 4).astype(F32).astype(BF16)
    wide = dot(levels, ops_v[640:672, 0:CZ]).astype(BF16)
    thr[...] = jnp.concatenate([dot(ops_v[672 + 256 * h : 928 + 256 * h, 0:CZ], wide) for h in range(2)]).reshape(STEPS, CX // 4, CY, CZ)
    for s in range(2):
        send_forward(s)

    load(6, trio, trio).wait()
    for copy in points_in:
        copy.wait()

    def weights(x, carry):
        over = 1.0 / (1.0 + damp_v[x])
        wa[x] = 2.0 * over
        wb[x] = (1.0 - damp_v[x]) * over
        we[x] = cour_v[x] * over
        return carry

    lax.fori_loop(0, CX, weights, 0, unroll=2)

    row = lax.broadcasted_iota(jnp.int32, (ROWS, RECS), 0)
    rows_hot = jnp.where(row == cell_v[...] // CZ, 1.0, 0.0).astype(BF16)
    rows_hot = jnp.concatenate([rows_hot, rows_hot], axis=1)
    at_lane = lax.broadcasted_iota(jnp.int32, (CZ, RECS), 0) == cell_v[...] % CZ
    for s in range(STEPS):
        lanes_hot = jnp.where(at_lane, data_v[s : s + 1, :], 0.0)
        lanes_hot = jnp.concatenate(split(lanes_hot), axis=1)
        spread = lax.dot_general(
            rows_hot, lanes_hot, (((1,), (1,)), ((), ())), preferred_element_type=F32
        )
        inj[s] = spread.reshape(CX, CY, CZ) * (0.5 * wa[...])

    adjoint_own(0)
    for s in range(STEPS):
        adjoint_far(s)
        if s < STEPS - 1:
            if s < 2:
                send_forward(2 + s)
            adjoint_own(s + 1)
            gradient(s)
            if s == STEPS - 2:
                gradient(s + 1)
    for d in range(3):
        drain(d)


def put_out(grad_v, last_v, before_v, grad_o, last_o, before_o, sem):
    pairs = ((grad_v, grad_o), (last_v, last_o), (before_v, before_o))
    copies = [pltpu.make_async_copy(v, o, sem.at[n]) for n, (v, o) in enumerate(pairs)]
    for copy in copies:
        copy.start()
    for copy in copies:
        copy.wait()


def local(coef, keep, courant, damp, adj_next, adj_now, rec_cell, rec_data):
    shape = (CX, CY, CZ)
    block = jax.ShapeDtypeStruct(shape, F32)
    ops = tables()
    vmem = pltpu.VMEM
    scratch = [
        vmem((8, 24, 48, CZ), F32),
        vmem((STEPS,) + shape, F32),
        vmem((STEPS, CX // 4, CY // 4, CZ // 4), jnp.int32),
        vmem((2, CX, 8, CZ), F32), vmem((3,) + shape, F32),
        vmem((1, RECS), jnp.int32), vmem((STEPS, RECS), F32), vmem(ops.shape, BF16),
        vmem(shape, F32), vmem(shape, F32), vmem(shape, F32),
        vmem((STEPS,) + shape, F32),
        vmem((STEPS, CX // 4, CY, CZ), F32),
        vmem(shape, F32),
        vmem((8, 2, 4, CY, CZ), F32),
        vmem((8, 2, 64, CZ), F32), vmem((8, 2, PIECES, 16 + PART, CZ), F32),
        vmem((8, 2, 16, CZ), F32), vmem((8, 2, 16, CZ), F32),
        pltpu.SemaphoreType.DMA((9,)),
        pltpu.SemaphoreType.DMA((3, 2)), pltpu.SemaphoreType.DMA((2, 2, 2 + PIECES)),
        pltpu.SemaphoreType.DMA((STEPS, 3, 2)),
    ]
    vmem_spec = pl.BlockSpec(memory_space=pltpu.VMEM)
    hbm_spec = pl.BlockSpec(memory_space=pltpu.HBM)
    results = pl.pallas_call(
        kernel,
        out_shape=(vmem(shape, F32),) * 3,
        in_specs=[hbm_spec] * 9,
        out_specs=(vmem_spec,) * 3,
        scratch_shapes=scratch,
        compiler_params=pltpu.CompilerParams(
            collective_id=0, has_side_effects=True, vmem_limit_bytes=67043328 - 3 * 4 * CX * CY * CZ
        ),
        name="adjoint_window",
    )(
        coef, keep, courant, damp, adj_next, adj_now,
        rec_cell.reshape(1, RECS), rec_data.reshape(STEPS, RECS),
        jnp.asarray(ops),
    )
    return pl.pallas_call(
        put_out,
        out_shape=(block,) * 3,
        in_specs=[pl.BlockSpec(memory_space=pl.ANY)] * 3,
        out_specs=(hbm_spec,) * 3,
        scratch_shapes=[pltpu.SemaphoreType.DMA((3,))],
        compiler_params=pltpu.CompilerParams(vmem_limit_bytes=1024 * 1024),
        name="put_out",
    )(*results)


def solution(mesh):
    field = P("gx", "gy", "gz")
    in_specs = (
        P(None, "gx", "gy", "gz"), P(None, "gx", "gy", "gz"),
        field, field, field, field,
        P("gx", "gy", "gz", None), P("gx", "gy", "gz", None, None),
    )
    return jax.shard_map(
        local, mesh=mesh, in_specs=in_specs, out_specs=(field,) * 3, check_vma=False
    )
```

```python
import functools

import jax
import jax.numpy as jnp
import numpy as np
from jax import lax
from jax.experimental import pallas as pl
from jax.experimental.pallas import tpu as pltpu
from jax.sharding import PartitionSpec as P

STAR = (-205.0 / 72.0, 8.0 / 5.0, -1.0 / 5.0, 8.0 / 315.0, -1.0 / 560.0)
CX, CY, CZ, STEPS, RECS = 16, 32, 128, 4, 128
ROWS = CX * CY
UNROLL = 16
AXES = ("gx", "gy", "gz")
MESH = pl.DeviceIdType.MESH
F32, BF16 = jnp.float32, jnp.bfloat16


def split_np(table):
    high = table.astype(np.float32).astype(jnp.bfloat16)
    low = (table - high.astype(np.float64)).astype(np.float32).astype(jnp.bfloat16)
    return high, low


def tables():
    freq, place = np.arange(4)[:, None], np.arange(4)[None, :]
    dct = np.where(freq == 0, 0.5, np.sqrt(0.5)) * np.cos(np.pi * (2 * place + 1) * freq / 8)
    along_z = np.kron(np.eye(CZ // 4), dct)
    along_xy = np.kron(dct.T, np.kron(np.eye(CY // 4), dct.T))
    gap = np.abs(np.arange(CZ)[:, None] - np.arange(CZ)[None, :])
    taps = np.select([gap == k for k in range(1, 5)], STAR[1:], 0.0)
    taps_hl = np.concatenate(split_np(taps), axis=1)
    z_hl = np.concatenate(split_np(along_z), axis=1)
    decode_xy = np.concatenate(split_np(along_xy), axis=1)
    spread_z = np.kron(np.eye(CZ // 4), np.ones((1, 4)))
    spread_y = np.kron(np.eye(STEPS * CX // 4), np.kron(np.eye(CY // 4), np.ones((4, 1))))
    spread = np.concatenate([spread_z, spread_y]).astype(jnp.bfloat16)
    spread = np.pad(spread, ((0, 0), (0, CZ)))
    return np.concatenate([taps_hl, taps_hl, z_hl, z_hl, decode_xy, spread])


def split(value):
    high = value.astype(BF16)
    low = (value - high.astype(F32)).astype(BF16)
    return high, low


def dot(a, b):
    return lax.dot_general(a, b, (((1,), (0,)), ((), ())), preferred_element_type=F32)


def halves(value):
    return value[:, :CZ] + value[:, CZ:]


def kernel(
    coef, keep, cour, damp, nxt, now, cell, data, ops,
    grad_o, last_o, before_o,
    F, cin, kin, edge_v, trio, cell_v, data_v, ops_v,
    wa, wb, we, inj, thr, Z, XH, YP, YH, CP, XC, ZP, ZH,
    load_sem, send_sem, step_sem, row_sem, forward_sem,
):
    me = [lax.axis_index(axis) for axis in AXES]
    size = [lax.axis_size(axis) for axis in AXES]
    has = [(me[d] > 0, me[d] < size[d] - 1) for d in range(3)]
    other = [({AXES[d]: me[d] - 1}, {AXES[d]: me[d] + 1}) for d in range(3)]

    barrier = pltpu.get_barrier_semaphore()
    for d in range(3):
        for side in range(2):
            @pl.when(has[d][side])
            def _():
                pl.semaphore_signal(
                    barrier, inc=1, device_id=other[d][side], device_id_type=MESH
                )

    def load(n, src, dst):
        return pltpu.make_async_copy(src, dst, load_sem.at[n])

    edges = [load(n, now.at[:, pl.ds(24 * n, 8)], edge_v.at[n]) for n in range(2)]
    first = load(2, now, F.at[0, pl.ds(4, CX), pl.ds(8, CY)])
    tables_in = [load(3, ops, ops_v), load(4, keep, kin), load(5, coef, cin)]
    points_in = [load(7, cell, cell_v), load(8, data, data_v)]
    fields_in = [load(6, src, trio.at[n]) for n, src in enumerate((cour, damp, nxt))]
    cour_v, damp_v, next_v = (trio.at[n] for n in range(3))
    for copy in edges + [first]:
        copy.start()

    def clear(f, carry):
        F[f, 0:4] = jnp.zeros((4, 48, CZ), F32)
        F[f, 20:24] = jnp.zeros((4, 48, CZ), F32)
        F[f, 4:20, 0:8] = jnp.zeros((CX, 8, CZ), F32)
        F[f, 4:20, 40:48] = jnp.zeros((CX, 8, CZ), F32)
        for side in range(2):
            YH[f, side, 0:8] = jnp.zeros((8, CZ), F32)
            YH[f, side, 72:80] = jnp.zeros((8, CZ), F32)

            @pl.when(jnp.logical_not(has[0][side]))
            def _():
                XH[f, side] = jnp.zeros((4, CY, CZ), F32)

            @pl.when(jnp.logical_not(has[1][side]))
            def _():
                YH[f, side, 8:72] = jnp.zeros((64, CZ), F32)

            @pl.when(jnp.logical_not(has[2][side]))
            def _():
                ZH[f, side] = jnp.zeros((16, CZ), F32)

        return carry

    lax.fori_loop(0, 8, clear, 0)
    for side in range(2):
        for f in range(STEPS - 1):
            CP[f, side, 0:8] = jnp.zeros((8, CZ), F32)
            CP[f, side, 72:80] = jnp.zeros((8, CZ), F32)

        @pl.when(jnp.logical_not(has[1][side]))
        def _():
            YH[8, side, 8:72] = jnp.zeros((64, CZ), F32)

    lane = lax.broadcasted_iota(jnp.int32, (8, CZ), 1)
    sub = lax.broadcasted_iota(jnp.int32, (8, CZ), 0)
    near_low = [None] + [jnp.where(sub < k, STAR[k], 0.0).astype(F32) for k in range(1, 5)]
    across = [
        [None] + [jnp.where(sub % 4 >= 4 - k, STAR[k], 0.0).astype(F32) for k in range(1, 5)],
        [None] + [jnp.where(sub % 4 < k, STAR[k], 0.0).astype(F32) for k in range(1, 5)],
    ]
    near_high = [None] + [jnp.where(sub >= 8 - k, STAR[k], 0.0).astype(F32) for k in range(1, 5)]

    def faces(f, d, side, some=slice(None)):
        if d == 0:
            start = 4 if side == 0 else CX
            rows = ((8, 16), (0, 8), (24, 8)) if f < STEPS else ((0, CY),)
            pairs = [
                (
                    F.at[f, pl.ds(start, 4), pl.ds(8 + row, count)],
                    XH.at[f, 1 - side, slice(None), pl.ds(row, count)],
                )
                for row, count in rows
            ]
        elif d == 1:
            pairs = [
                (YP.at[f, side, pl.ds(row, 16)], YH.at[f, 1 - side, pl.ds(8 + row, 16)])
                for row in range(0, 64, 16)
            ]
        else:
            pairs = [(ZP.at[f, side], ZH.at[f, 1 - side])]
        return [
            copy_to(f, d, side, src, dst) for src, dst in pairs[some]
        ]

    def copy_to(f, d, side, src, dst):
        if d == 1:
            landed = row_sem.at[f, 1 - side]
        elif f < STEPS:
            landed = step_sem.at[f % 2, d // 2, 1 - side]
        else:
            landed = forward_sem.at[f - STEPS, d // 2, 1 - side]
        return pltpu.make_async_remote_copy(
            src_ref=src,
            dst_ref=dst,
            send_sem=send_sem.at[d, side],
            recv_sem=landed,
            device_id=other[d][side],
            device_id_type=MESH,
        )

    def whole(f, d, side):
        from_ref, to_ref = ((XH, XH), (YP, YP), (ZP, ZH))[d]
        return copy_to(f, d, side, from_ref.at[f, side], to_ref.at[f, 1 - side])

    def each_side(d, act):
        for side in range(2):
            @pl.when(has[d][side])
            def _():
                act(side)

    def send(f, d, some=slice(None)):
        each_side(d, lambda side: [copy.start() for copy in faces(f, d, side, some)])

    def arrive(f, d):
        each_side(d, lambda side: whole(f, d, 1 - side).wait_recv())

    def drain(d):
        every = (XH, YP, ZP)[d]
        each_side(
            d, lambda side: copy_to(0, d, side, every.at[:, side], every.at[:, side]).wait_send()
        )

    def pack_rows(f):
        def pack_y(p, carry):
            for side, row in ((0, 8), (1, 36)):
                two = [F[f, 4 + 2 * p + q, row : row + 4, :] for q in range(2)]
                YP[f, side, pl.ds(pl.multiple_of(8 * p, 8), 8), :] = jnp.concatenate(two, axis=0)
            return carry

        lax.fori_loop(0, 8, pack_y, 0, unroll=True)

    def pack_lanes(f):
        def pack_z(q, kept):
            kept = list(kept)
            for tile in range(4):
                i = 4 * q + tile
                here = lane // 4 == i
                for half in range(2):
                    value = F[f, 4 + 8 * half + q, 8 + 8 * tile : 16 + 8 * tile, :]
                    low = pltpu.roll(value, 4 * i, 1)
                    high = pltpu.roll(value, (4 * i + 4) % CZ, 1)
                    kept[half] = jnp.where(here, low, kept[half])
                    kept[2 + half] = jnp.where(here, high, kept[2 + half])
            return tuple(kept)

        zero = jnp.zeros((8, CZ), F32)
        kept = lax.fori_loop(0, 8, pack_z, (zero,) * 4, unroll=True)
        for side in range(2):
            for half in range(2):
                ZP[f, side, 8 * half : 8 * half + 8, :] = kept[2 * side + half]

    def own_z(f):
        value = F[f, 4:20, 8:40, :].reshape(ROWS, CZ)
        return halves(dot(jnp.concatenate(split(value), axis=1), ops_v[0:256]))

    def far_z(f):
        member = lane % 4
        out = []
        for half in range(2):
            low = ZH[f, 0, 8 * half : 8 * half + 8, :]
            high = ZH[f, 1, 8 * half : 8 * half + 8, :]
            low_sum = STAR[4] * low
            high_sum = STAR[4] * high
            for k in range(1, 4):
                gap = 4 - k
                low_sum = low_sum + jnp.where(
                    member < k, STAR[k] * pltpu.roll(low, CZ - gap, 1), 0.0
                )
                high_sum = high_sum + jnp.where(
                    member >= gap, STAR[k] * pltpu.roll(high, gap, 1), 0.0
                )
            out.append((low_sum, high_sum))
        return out

    def add_z(f, target, scale):
        packed = far_z(f)
        for v in range(64):
            half, i = divmod(v, 32)
            low = pltpu.roll(packed[half][0], (CZ - 4 * i) % CZ, 1)
            high = pltpu.roll(packed[half][1], (252 - 4 * i) % CZ, 1)
            value = jnp.where(lane < 4, low, jnp.where(lane >= CZ - 4, high, 0.0))
            x, row = v // 4, 8 * (v % 4)
            at = (x, slice(row, row + 8))
            target[at] = target[at] + scale(*at) * value

    def add_x(f, target, scale):
        for i in range(4):
            low = sum(STAR[k] * XH[f, 0, 4 + i - k] for k in range(i + 1, 5))
            high = sum(STAR[4 + m - i] * XH[f, 1, m] for m in range(i + 1))
            target[i] = target[i] + scale(i) * low
            target[12 + i] = target[12 + i] + scale(12 + i) * high

    def near_y(f, x):
        at = 4 * x
        low = sum(near_low[k] * YH[f, 0, 12 + at - k : 20 + at - k] for k in range(1, 5))
        high = sum(near_high[k] * YH[f, 1, at + k : at + k + 8] for k in range(1, 5))
        return low, high

    def own_star(f, x):
        total = (3.0 * STAR[0]) * F[f, 4 + x, 8:40, :] + Z[x]
        for k in range(1, 5):
            pairs = F[f, 4 + x + k, 8:40, :] + F[f, 4 + x - k, 8:40, :]
            pairs = pairs + F[f, 4 + x, 8 + k : 40 + k, :] + F[f, 4 + x, 8 - k : 40 - k, :]
            total = total + STAR[k] * pairs
        return total

    def target_of(s):
        return last_o if s == STEPS - 1 else F.at[s + 1, pl.ds(4, CX), pl.ds(8, CY)]

    def adjoint_own(s):
        Z[...] = own_z(s).reshape(CX, CY, CZ)
        target = target_of(s)

        def step(x, carry):
            later = next_v[x] if s == 0 else F[s - 1, 4 + x, 8:40, :]
            current = F[s, 4 + x, 8:40, :]
            target[x] = wa[x] * current - wb[x] * later + we[x] * own_star(s, x) + inj[s, x]
            if s == STEPS - 1:
                before_o[x] = current
            return carry

        lax.fori_loop(0, CX, step, 0, unroll=UNROLL)

    def send_partial(f, pieces):
        target = target_of(f - 1)
        for n in pieces:
            for p in (2 * n, 2 * n + 1):
                for side, row in ((0, 0), (1, 28)):
                    two = [target[2 * p + q, row : row + 4, :] for q in range(2)]
                    YP[f, side, 8 * p : 8 * p + 8] = jnp.concatenate(two, axis=0)
        for n in pieces:
            send(f, 1, slice(n, n + 1))

    def step_scale(*at):
        return we[at]

    def adjoint_near(s):
        target = target_of(s)
        sends = s < STEPS - 1
        arrive(s, 2)
        add_z(s, target, step_scale)
        if sends:
            send_partial(s + 1, (1, 2))
        arrive(s, 0)
        add_x(s, target, step_scale)
        if sends:
            send_partial(s + 1, (0, 3))
            send(s + 1, 0, slice(0, 1))

    def cross(f):
        for p in range(8):
            at = 8 + 8 * p
            for side in range(2):
                total = 0.0
                for k in range(1, 5):
                    move = k - 4 if side == 0 else 4 - k
                    part = CP[f - 1, side, at + move : at + move + 8]
                    total = total + across[side][k] * part
                XC[side, 8 * p : 8 * p + 8] = YH[8, side, at : at + 8] * total

    def adjoint_rows(s):
        target = target_of(s)
        sends = s < STEPS - 1
        arrive(s, 1)
        if s > 0:
            for side in range(2):
                YH[s, side, 8:72] = YH[s, side, 8:72] + XC[side]
        for p in range(8):
            lows, highs = [], []
            for x in (2 * p, 2 * p + 1):
                low, high = near_y(s, x)
                low = target[x, 0:8] + we[x, 0:8] * low
                high = target[x, 24:32] + we[x, 24:32] * high
                lows.append(low[0:4])
                highs.append(high[4:8])
                target[x, 0:8] = low
                target[x, 24:32] = high
            if s < STEPS - 2:
                CP[s + 1, 0, 8 + 8 * p : 16 + 8 * p] = jnp.concatenate(lows, axis=0)
                CP[s + 1, 1, 8 + 8 * p : 16 + 8 * p] = jnp.concatenate(highs, axis=0)
        if sends:
            send(s + 1, 0, slice(1, 3))
            pack_lanes(s + 1)
            send(s + 1, 2)

    def decode(s):
        level = (
            lax.broadcasted_iota(jnp.int32, (CY, CZ), 0) % 4
            + lax.broadcasted_iota(jnp.int32, (CY, CZ), 1) % 4
        ).astype(F32)
        masked = [
            jnp.where(level + float(x % 4) < thr[s, x // 4], cin[s, x], 0.0) for x in range(CX)
        ]
        value = jnp.concatenate(masked, axis=0)
        along_z = halves(dot(jnp.concatenate(split(value), axis=1), ops_v[256:512]))
        for g in range(CX // 4):
            both = jnp.concatenate(split(along_z[CZ * g : CZ * g + CZ]), axis=1)
            out = halves(dot(ops_v[512:640], jnp.concatenate([both, both], axis=0)))
            F[4 + s, 4 + 4 * g : 8 + 4 * g, 8:40, :] = out.reshape(4, CY, CZ)

    def gradient_own(s):
        Z[...] = own_z(4 + s).reshape(CX, CY, CZ)

        def step(x, carry):
            value = cour_v[x] * F[s, 4 + x, 8:40, :] * own_star(4 + s, x)
            grad_o[x] = value if s == 0 else grad_o[x] + value
            return carry

        lax.fori_loop(0, CX, step, 0, unroll=UNROLL)

    def gradient_far(s):
        f = 4 + s
        current = F.at[s, pl.ds(4, CX), pl.ds(8, CY)]

        def scale(*at):
            return cour_v[at] * current[at]

        arrive(f, 2)
        add_z(f, grad_o, scale)
        arrive(f, 0)
        add_x(f, grad_o, scale)
        arrive(f, 1)
        for x in range(CX):
            low, high = near_y(f, x)
            top, end = slice(0, 8), slice(24, 32)
            grad_o[x, top] = grad_o[x, top] + scale(x, top) * low
            grad_o[x, end] = grad_o[x, end] + scale(x, end) * high

    def prepare(s):
        decode(s)
        pack_rows(4 + s)
        pack_lanes(4 + s)

    def post(s):
        for d in (1, 0, 2):
            send(4 + s, d)

    for copy in edges:
        copy.wait()
    for copy in tables_in + fields_in + points_in:
        copy.start()
    for p in range(8):
        for side in range(2):
            two = [edge_v[side, 2 * p + q, 4 * side : 4 * side + 4, :] for q in range(2)]
            rows = jnp.concatenate(two, axis=0)
            YP[0, side, 8 * p : 8 * p + 8, :] = rows
            CP[0, side, 8 + 8 * p : 16 + 8 * p, :] = rows
    peers = sum(there.astype(jnp.int32) for pair in has for there in pair)
    pl.semaphore_wait(barrier, peers)
    send(0, 1)
    first.wait()
    send(0, 0)
    pack_lanes(0)
    send(0, 2)

    load(6, trio, trio).wait()
    for copy in points_in:
        copy.wait()

    def weights(x, carry):
        over = 1.0 / (1.0 + damp_v[x])
        wa[x] = 2.0 * over
        wb[x] = (1.0 - damp_v[x]) * over
        we[x] = cour_v[x] * over
        return carry

    lax.fori_loop(0, CX, weights, 0, unroll=2)

    for p in range(8):
        for side in range(2):
            row = 28 * side
            two = [we[2 * p + q, row : row + 4, :] for q in range(2)]
            YP[8, side, 8 * p : 8 * p + 8] = jnp.concatenate(two, axis=0)
    send(8, 1)

    row = lax.broadcasted_iota(jnp.int32, (ROWS, RECS), 0)
    rows_hot = jnp.where(row == cell_v[...] // CZ, 1.0, 0.0).astype(BF16)
    rows_hot = jnp.concatenate([rows_hot, rows_hot], axis=1)
    at_lane = lax.broadcasted_iota(jnp.int32, (CZ, RECS), 0) == cell_v[...] % CZ
    for s in range(STEPS):
        lanes_hot = jnp.where(at_lane, data_v[s : s + 1, :], 0.0)
        lanes_hot = jnp.concatenate(split(lanes_hot), axis=1)
        spread = lax.dot_general(
            rows_hot, lanes_hot, (((1,), (1,)), ((), ())), preferred_element_type=F32
        )
        inj[s] = spread.reshape(CX, CY, CZ) * (0.5 * wa[...])

    for copy in tables_in:
        copy.wait()
    levels = kin[...].reshape(STEPS * (CX // 4) * (CY // 4), CZ // 4).astype(F32).astype(BF16)
    wide = dot(levels, ops_v[640:672, 0:CZ]).astype(BF16)
    thr[...] = jnp.concatenate([dot(ops_v[672 + 256 * h : 928 + 256 * h, 0:CZ], wide) for h in range(2)]).reshape(STEPS, CX // 4, CY, CZ)

    prepare(0)
    post(0)
    adjoint_own(0)
    prepare(1)
    adjoint_near(0)
    adjoint_rows(0)
    post(1)
    arrive(8, 1)

    adjoint_own(1)
    cross(1)
    prepare(2)
    gradient_own(0)
    adjoint_near(1)
    adjoint_rows(1)
    post(2)

    adjoint_own(2)
    cross(2)
    prepare(3)
    post(3)
    gradient_own(1)
    gradient_far(0)
    adjoint_near(2)
    adjoint_rows(2)

    adjoint_own(3)
    cross(3)
    gradient_own(2)
    gradient_own(3)
    gradient_far(1)
    gradient_far(2)
    adjoint_near(3)
    gradient_far(3)
    adjoint_rows(3)
    for d in range(3):
        drain(d)


def put_out(grad_v, last_v, before_v, grad_o, last_o, before_o, sem):
    pairs = ((grad_v, grad_o), (last_v, last_o), (before_v, before_o))
    copies = [pltpu.make_async_copy(v, o, sem.at[n]) for n, (v, o) in enumerate(pairs)]
    for copy in copies:
        copy.start()
    for copy in copies:
        copy.wait()


def local(coef, keep, courant, damp, adj_next, adj_now, rec_cell, rec_data):
    shape = (CX, CY, CZ)
    block = jax.ShapeDtypeStruct(shape, F32)
    ops = tables()
    vmem = pltpu.VMEM
    scratch = [
        vmem((8, 24, 48, CZ), F32),
        vmem((STEPS,) + shape, F32),
        vmem((STEPS, CX // 4, CY // 4, CZ // 4), jnp.int32),
        vmem((2, CX, 8, CZ), F32), vmem((3,) + shape, F32),
        vmem((1, RECS), jnp.int32), vmem((STEPS, RECS), F32), vmem(ops.shape, BF16),
        vmem(shape, F32), vmem(shape, F32), vmem(shape, F32),
        vmem((STEPS,) + shape, F32),
        vmem((STEPS, CX // 4, CY, CZ), F32),
        vmem(shape, F32),
        vmem((8, 2, 4, CY, CZ), F32),
        vmem((9, 2, 64, CZ), F32), vmem((9, 2, 80, CZ), F32),
        vmem((STEPS - 1, 2, 80, CZ), F32), vmem((2, 64, CZ), F32),
        vmem((8, 2, 16, CZ), F32), vmem((8, 2, 16, CZ), F32),
        pltpu.SemaphoreType.DMA((9,)),
        pltpu.SemaphoreType.DMA((3, 2)), pltpu.SemaphoreType.DMA((2, 2, 2)),
        pltpu.SemaphoreType.DMA((9, 2)), pltpu.SemaphoreType.DMA((STEPS, 2, 2)),
    ]
    vmem_spec = pl.BlockSpec(memory_space=pltpu.VMEM)
    hbm_spec = pl.BlockSpec(memory_space=pltpu.HBM)
    results = pl.pallas_call(
        kernel,
        out_shape=(vmem(shape, F32),) * 3,
        in_specs=[hbm_spec] * 9,
        out_specs=(vmem_spec,) * 3,
        scratch_shapes=scratch,
        compiler_params=pltpu.CompilerParams(
            collective_id=0, has_side_effects=True, vmem_limit_bytes=67043328 - 3 * 4 * CX * CY * CZ
        ),
        name="adjoint_window",
    )(
        coef, keep, courant, damp, adj_next, adj_now,
        rec_cell.reshape(1, RECS), rec_data.reshape(STEPS, RECS),
        jnp.asarray(ops),
    )
    return pl.pallas_call(
        put_out,
        out_shape=(block,) * 3,
        in_specs=[pl.BlockSpec(memory_space=pl.ANY)] * 3,
        out_specs=(hbm_spec,) * 3,
        scratch_shapes=[pltpu.SemaphoreType.DMA((3,))],
        compiler_params=pltpu.CompilerParams(vmem_limit_bytes=1024 * 1024),
        name="put_out",
    )(*results)


def solution(mesh):
    field = P("gx", "gy", "gz")
    in_specs = (
        P(None, "gx", "gy", "gz"), P(None, "gx", "gy", "gz"),
        field, field, field, field,
        P("gx", "gy", "gz", None), P("gx", "gy", "gz", None, None),
    )
    return jax.shard_map(
        local, mesh=mesh, in_specs=in_specs, out_specs=(field,) * 3, check_vma=False
    )
```

```python
import functools

import jax
import jax.numpy as jnp
import numpy as np
from jax import lax
from jax.experimental import pallas as pl
from jax.experimental.pallas import tpu as pltpu
from jax.sharding import PartitionSpec as P

STAR = (-205.0 / 72.0, 8.0 / 5.0, -1.0 / 5.0, 8.0 / 315.0, -1.0 / 560.0)
CX, CY, CZ, STEPS, RECS = 16, 32, 128, 4, 128
ROWS = CX * CY
UNROLL = 16
AXES = ("gx", "gy", "gz")
MESH = pl.DeviceIdType.MESH
F32, BF16 = jnp.float32, jnp.bfloat16


def split_np(table):
    high = table.astype(np.float32).astype(jnp.bfloat16)
    low = (table - high.astype(np.float64)).astype(np.float32).astype(jnp.bfloat16)
    return high, low


def tables():
    freq, place = np.arange(4)[:, None], np.arange(4)[None, :]
    dct = np.where(freq == 0, 0.5, np.sqrt(0.5)) * np.cos(np.pi * (2 * place + 1) * freq / 8)
    along_z = np.kron(np.eye(CZ // 4), dct)
    along_xy = np.kron(dct.T, np.kron(np.eye(CY // 4), dct.T))
    gap = np.abs(np.arange(CZ)[:, None] - np.arange(CZ)[None, :])
    taps = np.select([gap == k for k in range(1, 5)], STAR[1:], 0.0)
    taps_hl = np.concatenate(split_np(taps), axis=1)
    z_hl = np.concatenate(split_np(along_z), axis=1)
    decode_xy = np.concatenate(split_np(along_xy), axis=1)
    spread_z = np.kron(np.eye(CZ // 4), np.ones((1, 4)))
    spread_y = np.kron(np.eye(STEPS * CX // 4), np.kron(np.eye(CY // 4), np.ones((4, 1))))
    spread = np.concatenate([spread_z, spread_y]).astype(jnp.bfloat16)
    spread = np.pad(spread, ((0, 0), (0, CZ)))
    return np.concatenate([taps_hl, taps_hl, z_hl, z_hl, decode_xy, spread])


def split(value):
    high = value.astype(BF16)
    low = (value - high.astype(F32)).astype(BF16)
    return high, low


def dot(a, b):
    return lax.dot_general(a, b, (((1,), (0,)), ((), ())), preferred_element_type=F32)


def halves(value):
    return value[:, :CZ] + value[:, CZ:]


def kernel(
    coef, keep, cour, damp, nxt, now, cell, data, ops,
    grad_o, last_o, before_o,
    F, cin, kin, edge_v, trio, cell_v, data_v, ops_v,
    wa, wb, we, inj, thr, Z, XH, YP, YH, CP, XC, XP, XM, XL, XT, ZP, ZH,
    load_sem, send_sem, step_sem, row_sem, forward_sem, edge_sem,
):
    me = [lax.axis_index(axis) for axis in AXES]
    size = [lax.axis_size(axis) for axis in AXES]
    has = [(me[d] > 0, me[d] < size[d] - 1) for d in range(3)]
    other = [({AXES[d]: me[d] - 1}, {AXES[d]: me[d] + 1}) for d in range(3)]

    barrier = pltpu.get_barrier_semaphore()
    for d in (1, 0, 2):
        for side in range(2):
            @pl.when(has[d][side])
            def _():
                pl.semaphore_signal(
                    barrier, inc=1, device_id=other[d][side], device_id_type=MESH
                )

    def load(n, src, dst):
        return pltpu.make_async_copy(src, dst, load_sem.at[n])

    edges = [load(n, now.at[:, pl.ds(24 * n, 8)], edge_v.at[n]) for n in range(2)]
    first = load(2, now, F.at[0, pl.ds(4, CX), pl.ds(8, CY)])
    tables_in = [load(3, ops, ops_v), load(4, keep, kin), load(5, coef, cin)]
    points_in = [load(7, cell, cell_v), load(8, data, data_v)]
    fields_in = [load(6, src, trio.at[n]) for n, src in enumerate((cour, damp, nxt))]
    cour_v, damp_v, next_v = (trio.at[n] for n in range(3))
    for copy in edges + [first]:
        copy.start()

    def clear(f, carry):
        F[f, 0:4] = jnp.zeros((4, 48, CZ), F32)
        F[f, 20:24] = jnp.zeros((4, 48, CZ), F32)
        F[f, 4:20, 0:8] = jnp.zeros((CX, 8, CZ), F32)
        F[f, 4:20, 40:48] = jnp.zeros((CX, 8, CZ), F32)
        for side in range(2):
            YH[f, side, 0:8] = jnp.zeros((8, CZ), F32)
            YH[f, side, 72:80] = jnp.zeros((8, CZ), F32)

            @pl.when(jnp.logical_not(has[0][side]))
            def _():
                XH[f, side] = jnp.zeros((4, CY, CZ), F32)

            @pl.when(jnp.logical_not(has[1][side]))
            def _():
                YH[f, side, 8:72] = jnp.zeros((64, CZ), F32)

            @pl.when(jnp.logical_not(has[2][side]))
            def _():
                ZH[f, side] = jnp.zeros((16, CZ), F32)

        return carry

    lax.fori_loop(0, 8, clear, 0)
    for side in range(2):
        XT[side] = jnp.zeros((4, 16, CZ), F32)
        for f in range(1, STEPS):
            for row in (0, 24):
                XH[f, side, :, row : row + 8] = jnp.zeros((4, 8, CZ), F32)
        for f in range(STEPS):
            CP[f, side, 0:8] = jnp.zeros((8, CZ), F32)
            CP[f, side, 72:80] = jnp.zeros((8, CZ), F32)

        @pl.when(jnp.logical_not(has[1][side]))
        def _():
            YH[8, side, 8:72] = jnp.zeros((64, CZ), F32)

    lane = lax.broadcasted_iota(jnp.int32, (8, CZ), 1)
    sub = lax.broadcasted_iota(jnp.int32, (8, CZ), 0)
    near_low = [None] + [jnp.where(sub < k, STAR[k], 0.0).astype(F32) for k in range(1, 5)]
    across = [
        [None] + [jnp.where(sub % 4 >= 4 - k, STAR[k], 0.0).astype(F32) for k in range(1, 5)],
        [None] + [jnp.where(sub % 4 < k, STAR[k], 0.0).astype(F32) for k in range(1, 5)],
    ]
    near_high = [None] + [jnp.where(sub >= 8 - k, STAR[k], 0.0).astype(F32) for k in range(1, 5)]

    def faces(f, d, side, some=slice(None)):
        if d == 0 and 0 < f < STEPS:
            inner, there = pl.ds(8, 16), 1 - side
            pairs = [(F.at[f, pl.ds(4 + 12 * side, 4), pl.ds(16, 16)], XH.at[f, there, :, inner])]
            pairs += [(XP.at[f - 1, side, t], XM.at[f - 1, there, t]) for t in range(2)]
            row = pl.ds(8 + 48 * side, 16)
            pairs += [(CP.at[f, t, row], XL.at[f - 1, there, t]) for t in range(2)]
        elif d == 0:
            start = 4 if side == 0 else CX
            pairs = [(F.at[f, pl.ds(start, 4), pl.ds(8, CY)], XH.at[f, 1 - side])]
        elif d == 1:
            pairs = [
                (YP.at[f, side, pl.ds(row, 16)], YH.at[f, 1 - side, pl.ds(8 + row, 16)])
                for row in range(0, 64, 16)
            ]
        else:
            pairs = [(ZP.at[f, side], ZH.at[f, 1 - side])]
        return [
            copy_to(f, d, side, src, dst, n) for n, (src, dst) in list(enumerate(pairs))[some]
        ]

    def copy_to(f, d, side, src, dst, n=0):
        if d == 0 and n > 2:
            landed = edge_sem.at[f % 2, 1 - side]
        elif d == 1:
            landed = row_sem.at[f, 1 - side]
        elif f < STEPS:
            landed = step_sem.at[f % 2, d // 2, 1 - side]
        else:
            landed = forward_sem.at[f - STEPS, d // 2, 1 - side]
        return pltpu.make_async_remote_copy(
            src_ref=src,
            dst_ref=dst,
            send_sem=send_sem.at[d, side],
            recv_sem=landed,
            device_id=other[d][side],
            device_id_type=MESH,
        )

    def whole(f, d, side, n=0):
        from_ref, to_ref = ((XH, XH), (YP, YP), (ZP, ZH))[d]
        src, dst = from_ref.at[f, side], to_ref.at[f, 1 - side]
        if d == 0 and 0 < f < STEPS:
            src, dst = (ref.at[:, pl.ds(0, 8 if n else 24)] for ref in (src, dst))
        return copy_to(f, d, side, src, dst, n)

    def each_side(d, act):
        for side in range(2):
            @pl.when(has[d][side])
            def _():
                act(side)

    def send(f, d, some=slice(None)):
        each_side(d, lambda side: [copy.start() for copy in faces(f, d, side, some)])

    def arrive(f, d, n=0):
        each_side(d, lambda side: whole(f, d, 1 - side, n).wait_recv())

    def drain(d):
        every = (XH, YP, ZP)[d]
        each_side(
            d, lambda side: copy_to(0, d, side, every.at[:, side], every.at[:, side]).wait_send()
        )

    def pack_rows(f):
        def pack_y(p, carry):
            for side, row in ((0, 8), (1, 36)):
                two = [F[f, 4 + 2 * p + q, row : row + 4, :] for q in range(2)]
                YP[f, side, pl.ds(pl.multiple_of(8 * p, 8), 8), :] = jnp.concatenate(two, axis=0)
            return carry

        lax.fori_loop(0, 8, pack_y, 0, unroll=True)

    def pack_lanes(f):
        def pack_z(q, kept):
            kept = list(kept)
            for tile in range(4):
                i = 4 * q + tile
                here = lane // 4 == i
                for half in range(2):
                    value = F[f, 4 + 8 * half + q, 8 + 8 * tile : 16 + 8 * tile, :]
                    low = pltpu.roll(value, 4 * i, 1)
                    high = pltpu.roll(value, (4 * i + 4) % CZ, 1)
                    kept[half] = jnp.where(here, low, kept[half])
                    kept[2 + half] = jnp.where(here, high, kept[2 + half])
            return tuple(kept)

        zero = jnp.zeros((8, CZ), F32)
        kept = lax.fori_loop(0, 8, pack_z, (zero,) * 4, unroll=True)
        for side in range(2):
            for half in range(2):
                ZP[f, side, 8 * half : 8 * half + 8, :] = kept[2 * side + half]

    def own_z(f):
        value = F[f, 4:20, 8:40, :].reshape(ROWS, CZ)
        return halves(dot(jnp.concatenate(split(value), axis=1), ops_v[0:256]))

    def far_z(f):
        member = lane % 4
        out = []
        for half in range(2):
            low = ZH[f, 0, 8 * half : 8 * half + 8, :]
            high = ZH[f, 1, 8 * half : 8 * half + 8, :]
            low_sum = STAR[4] * low
            high_sum = STAR[4] * high
            for k in range(1, 4):
                gap = 4 - k
                low_sum = low_sum + jnp.where(
                    member < k, STAR[k] * pltpu.roll(low, CZ - gap, 1), 0.0
                )
                high_sum = high_sum + jnp.where(
                    member >= gap, STAR[k] * pltpu.roll(high, gap, 1), 0.0
                )
            out.append((low_sum, high_sum))
        return out

    def add_z(f, target, scale):
        packed = far_z(f)
        for v in range(64):
            half, i = divmod(v, 32)
            low = pltpu.roll(packed[half][0], (CZ - 4 * i) % CZ, 1)
            high = pltpu.roll(packed[half][1], (252 - 4 * i) % CZ, 1)
            value = jnp.where(lane < 4, low, jnp.where(lane >= CZ - 4, high, 0.0))
            x, row = v // 4, 8 * (v % 4)
            at = (x, slice(row, row + 8))
            target[at] = target[at] + scale(*at) * value

    def add_x(f, target, scale, parts=((0, CY),)):
        for start, stop in parts:
            rows = slice(start, stop)
            for i in range(4):
                low = sum(STAR[k] * XH[f, 0, 4 + i - k, rows] for k in range(i + 1, 5))
                high = sum(STAR[4 + m - i] * XH[f, 1, m, rows] for m in range(i + 1))
                target[i, rows] = target[i, rows] + scale(i, rows) * low
                target[12 + i, rows] = target[12 + i, rows] + scale(12 + i, rows) * high

    def near_y(f, x):
        at = 4 * x
        low = sum(near_low[k] * YH[f, 0, 12 + at - k : 20 + at - k] for k in range(1, 5))
        high = sum(near_high[k] * YH[f, 1, at + k : at + k + 8] for k in range(1, 5))
        return low, high

    def own_star(f, x):
        total = (3.0 * STAR[0]) * F[f, 4 + x, 8:40, :] + Z[x]
        for k in range(1, 5):
            pairs = F[f, 4 + x + k, 8:40, :] + F[f, 4 + x - k, 8:40, :]
            pairs = pairs + F[f, 4 + x, 8 + k : 40 + k, :] + F[f, 4 + x, 8 - k : 40 - k, :]
            total = total + STAR[k] * pairs
        return total

    def target_of(s):
        return last_o if s == STEPS - 1 else F.at[s + 1, pl.ds(4, CX), pl.ds(8, CY)]

    def adjoint_own(s):
        Z[...] = own_z(s).reshape(CX, CY, CZ)
        target = target_of(s)

        def step(x, carry):
            later = next_v[x] if s == 0 else F[s - 1, 4 + x, 8:40, :]
            current = F[s, 4 + x, 8:40, :]
            target[x] = wa[x] * current - wb[x] * later + we[x] * own_star(s, x) + inj[s, x]
            if s == STEPS - 1:
                before_o[x] = current
            return carry

        lax.fori_loop(0, CX, step, 0, unroll=UNROLL)

    def send_partial(f, pieces):
        target = target_of(f - 1)
        for n in pieces:
            for p in (2 * n, 2 * n + 1):
                for side, row in ((0, 0), (1, 28)):
                    two = [target[2 * p + q, row : row + 4, :] for q in range(2)]
                    YP[f, side, 8 * p : 8 * p + 8] = jnp.concatenate(two, axis=0)
        for n in pieces:
            send(f, 1, slice(n, n + 1))

    def step_scale(*at):
        return we[at]

    def adjoint_near(s):
        target = target_of(s)
        sends = s < STEPS - 1
        arrive(s, 2)
        add_z(s, target, step_scale)
        if sends:
            send_partial(s + 1, (1, 2))
        arrive(s, 0)
        if s > 0:
            each_side(0, lambda side: place(XM.at[s - 1, side], XH.at[s, side], ((0, 4), (1, 24))))
        add_x(s, target, step_scale)
        if sends:
            send(s + 1, 0, slice(0, 1))
            for side in range(2):
                for t, row in ((0, 4), (1, 24)):
                    for p in range(2):
                        two = [target[12 * side + 2 * p + q, row : row + 4, :] for q in range(2)]
                        XP[s, side, t, 8 * p : 8 * p + 8] = jnp.concatenate(two, axis=0)
            send(s + 1, 0, slice(1, 3))
        if s > 0:
            arrive(s, 0, 3)
            each_side(0, lambda side: place(XL.at[s - 1, side], XT.at[side], ((0, 0), (1, 12))))
            for t, rows in ((0, slice(0, 8)), (1, slice(24, 32))):
                own = slice(8 * t, 8 * t + 8)
                for i in range(4):
                    low = sum(STAR[k] * XT[0, 4 + i - k, own] for k in range(i + 1, 5))
                    high = sum(STAR[4 + m - i] * XT[1, m, own] for m in range(i + 1))
                    target[i, rows] = target[i, rows] + we[i, rows] * low
                    target[12 + i, rows] = target[12 + i, rows] + we[12 + i, rows] * high
        if sends:
            send_partial(s + 1, (0, 3))

    def place(packed, slabs, spots):
        for t, row in spots:
            for i in range(4):
                slabs[i, row : row + 4] = packed[t, 4 * i : 4 * i + 4]

    def cross(f):
        for p in range(8):
            at = 8 + 8 * p
            for side in range(2):
                total = 0.0
                for k in range(1, 5):
                    move = k - 4 if side == 0 else 4 - k
                    part = CP[f - 1, side, at + move : at + move + 8]
                    total = total + across[side][k] * part
                XC[side, 8 * p : 8 * p + 8] = YH[8, side, at : at + 8] * total

    def adjoint_rows(s):
        target = target_of(s)
        sends = s < STEPS - 1
        arrive(s, 1)
        if s > 0:
            for side in range(2):
                YH[s, side, 8:72] = YH[s, side, 8:72] + XC[side]
        for p in range(8):
            lows, highs = [], []
            for x in (2 * p, 2 * p + 1):
                low, high = near_y(s, x)
                low = target[x, 0:8] + we[x, 0:8] * low
                high = target[x, 24:32] + we[x, 24:32] * high
                lows.append(low[0:4])
                highs.append(high[4:8])
                target[x, 0:8] = low
                target[x, 24:32] = high
            if sends:
                CP[s + 1, 0, 8 + 8 * p : 16 + 8 * p] = jnp.concatenate(lows, axis=0)
                CP[s + 1, 1, 8 + 8 * p : 16 + 8 * p] = jnp.concatenate(highs, axis=0)
        if sends:
            send(s + 1, 0, slice(3, 5))
            pack_lanes(s + 1)
            send(s + 1, 2)

    def decode(s):
        level = (
            lax.broadcasted_iota(jnp.int32, (CY, CZ), 0) % 4
            + lax.broadcasted_iota(jnp.int32, (CY, CZ), 1) % 4
        ).astype(F32)
        masked = [
            jnp.where(level + float(x % 4) < thr[s, x // 4], cin[s, x], 0.0) for x in range(CX)
        ]
        value = jnp.concatenate(masked, axis=0)
        along_z = halves(dot(jnp.concatenate(split(value), axis=1), ops_v[256:512]))
        for g in range(CX // 4):
            both = jnp.concatenate(split(along_z[CZ * g : CZ * g + CZ]), axis=1)
            out = halves(dot(ops_v[512:640], jnp.concatenate([both, both], axis=0)))
            F[4 + s, 4 + 4 * g : 8 + 4 * g, 8:40, :] = out.reshape(4, CY, CZ)

    def gradient_own(s):
        Z[...] = own_z(4 + s).reshape(CX, CY, CZ)

        def step(x, carry):
            value = cour_v[x] * F[s, 4 + x, 8:40, :] * own_star(4 + s, x)
            grad_o[x] = value if s == 0 else grad_o[x] + value
            return carry

        lax.fori_loop(0, CX, step, 0, unroll=UNROLL)

    def gradient_far(s):
        f = 4 + s
        current = F.at[s, pl.ds(4, CX), pl.ds(8, CY)]

        def scale(*at):
            return cour_v[at] * current[at]

        arrive(f, 2)
        add_z(f, grad_o, scale)
        arrive(f, 0)
        add_x(f, grad_o, scale)
        arrive(f, 1)
        for x in range(CX):
            low, high = near_y(f, x)
            top, end = slice(0, 8), slice(24, 32)
            grad_o[x, top] = grad_o[x, top] + scale(x, top) * low
            grad_o[x, end] = grad_o[x, end] + scale(x, end) * high

    def prepare(s):
        decode(s)
        pack_rows(4 + s)
        pack_lanes(4 + s)

    def post(s):
        for d in (1, 0, 2):
            send(4 + s, d)

    for copy in edges:
        copy.wait()
    for copy in tables_in + fields_in + points_in:
        copy.start()
    for p in range(8):
        for side in range(2):
            two = [edge_v[side, 2 * p + q, 4 * side : 4 * side + 4, :] for q in range(2)]
            rows = jnp.concatenate(two, axis=0)
            YP[0, side, 8 * p : 8 * p + 8, :] = rows
            CP[0, side, 8 + 8 * p : 16 + 8 * p, :] = rows
    peers = sum(there.astype(jnp.int32) for pair in has for there in pair)
    pl.semaphore_wait(barrier, peers)
    send(0, 1)
    first.wait()
    send(0, 0)
    pack_lanes(0)
    send(0, 2)

    load(6, trio, trio).wait()
    for copy in points_in:
        copy.wait()

    def weights(x, carry):
        over = 1.0 / (1.0 + damp_v[x])
        wa[x] = 2.0 * over
        wb[x] = (1.0 - damp_v[x]) * over
        we[x] = cour_v[x] * over
        return carry

    lax.fori_loop(0, CX, weights, 0, unroll=2)

    for p in range(8):
        for side in range(2):
            row = 28 * side
            two = [we[2 * p + q, row : row + 4, :] for q in range(2)]
            YP[8, side, 8 * p : 8 * p + 8] = jnp.concatenate(two, axis=0)
    send(8, 1)

    row = lax.broadcasted_iota(jnp.int32, (ROWS, RECS), 0)
    rows_hot = jnp.where(row == cell_v[...] // CZ, 1.0, 0.0).astype(BF16)
    rows_hot = jnp.concatenate([rows_hot, rows_hot], axis=1)
    at_lane = lax.broadcasted_iota(jnp.int32, (CZ, RECS), 0) == cell_v[...] % CZ
    for s in range(STEPS):
        lanes_hot = jnp.where(at_lane, data_v[s : s + 1, :], 0.0)
        lanes_hot = jnp.concatenate(split(lanes_hot), axis=1)
        spread = lax.dot_general(
            rows_hot, lanes_hot, (((1,), (1,)), ((), ())), preferred_element_type=F32
        )
        inj[s] = spread.reshape(CX, CY, CZ) * (0.5 * wa[...])

    for copy in tables_in:
        copy.wait()
    levels = kin[...].reshape(STEPS * (CX // 4) * (CY // 4), CZ // 4).astype(F32).astype(BF16)
    wide = dot(levels, ops_v[640:672, 0:CZ]).astype(BF16)
    thr[...] = jnp.concatenate([dot(ops_v[672 + 256 * h : 928 + 256 * h, 0:CZ], wide) for h in range(2)]).reshape(STEPS, CX // 4, CY, CZ)

    prepare(0)
    post(0)
    adjoint_own(0)
    prepare(1)
    adjoint_near(0)
    adjoint_rows(0)
    post(1)
    arrive(8, 1)

    adjoint_own(1)
    cross(1)
    prepare(2)
    gradient_own(0)
    adjoint_near(1)
    adjoint_rows(1)
    post(2)

    adjoint_own(2)
    cross(2)
    prepare(3)
    post(3)
    gradient_own(1)
    gradient_far(0)
    adjoint_near(2)
    adjoint_rows(2)

    adjoint_own(3)
    cross(3)
    gradient_own(2)
    gradient_own(3)
    gradient_far(1)
    gradient_far(2)
    adjoint_near(3)
    gradient_far(3)
    adjoint_rows(3)
    for d in range(3):
        drain(d)


def put_out(grad_v, last_v, before_v, grad_o, last_o, before_o, sem):
    pairs = ((grad_v, grad_o), (last_v, last_o), (before_v, before_o))
    copies = [pltpu.make_async_copy(v, o, sem.at[n]) for n, (v, o) in enumerate(pairs)]
    for copy in copies:
        copy.start()
    for copy in copies:
        copy.wait()


def local(coef, keep, courant, damp, adj_next, adj_now, rec_cell, rec_data):
    shape = (CX, CY, CZ)
    block = jax.ShapeDtypeStruct(shape, F32)
    ops = tables()
    vmem = pltpu.VMEM
    scratch = [
        vmem((8, 24, 48, CZ), F32),
        vmem((STEPS,) + shape, F32),
        vmem((STEPS, CX // 4, CY // 4, CZ // 4), jnp.int32),
        vmem((2, CX, 8, CZ), F32), vmem((3,) + shape, F32),
        vmem((1, RECS), jnp.int32), vmem((STEPS, RECS), F32), vmem(ops.shape, BF16),
        vmem(shape, F32), vmem(shape, F32), vmem(shape, F32),
        vmem((STEPS,) + shape, F32),
        vmem((STEPS, CX // 4, CY, CZ), F32),
        vmem(shape, F32),
        vmem((8, 2, 4, CY, CZ), F32),
        vmem((9, 2, 64, CZ), F32), vmem((9, 2, 80, CZ), F32),
        vmem((STEPS, 2, 80, CZ), F32), vmem((2, 64, CZ), F32),
        vmem((STEPS - 1, 2, 2, 16, CZ), F32), vmem((STEPS - 1, 2, 2, 16, CZ), F32),
        vmem((STEPS - 1, 2, 2, 16, CZ), F32), vmem((2, 4, 16, CZ), F32),
        vmem((8, 2, 16, CZ), F32), vmem((8, 2, 16, CZ), F32),
        pltpu.SemaphoreType.DMA((9,)),
        pltpu.SemaphoreType.DMA((3, 2)), pltpu.SemaphoreType.DMA((2, 2, 2)),
        pltpu.SemaphoreType.DMA((9, 2)), pltpu.SemaphoreType.DMA((STEPS, 2, 2)),
        pltpu.SemaphoreType.DMA((2, 2)),
    ]
    vmem_spec = pl.BlockSpec(memory_space=pltpu.VMEM)
    hbm_spec = pl.BlockSpec(memory_space=pltpu.HBM)
    results = pl.pallas_call(
        kernel,
        out_shape=(vmem(shape, F32),) * 3,
        in_specs=[hbm_spec] * 9,
        out_specs=(vmem_spec,) * 3,
        scratch_shapes=scratch,
        compiler_params=pltpu.CompilerParams(
            collective_id=0, has_side_effects=True, vmem_limit_bytes=67043328 - 3 * 4 * CX * CY * CZ
        ),
        name="adjoint_window",
    )(
        coef, keep, courant, damp, adj_next, adj_now,
        rec_cell.reshape(1, RECS), rec_data.reshape(STEPS, RECS),
        jnp.asarray(ops),
    )
    return pl.pallas_call(
        put_out,
        out_shape=(block,) * 3,
        in_specs=[pl.BlockSpec(memory_space=pl.ANY)] * 3,
        out_specs=(hbm_spec,) * 3,
        scratch_shapes=[pltpu.SemaphoreType.DMA((3,))],
        compiler_params=pltpu.CompilerParams(vmem_limit_bytes=1024 * 1024),
        name="put_out",
    )(*results)


def solution(mesh):
    field = P("gx", "gy", "gz")
    in_specs = (
        P(None, "gx", "gy", "gz"), P(None, "gx", "gy", "gz"),
        field, field, field, field,
        P("gx", "gy", "gz", None), P("gx", "gy", "gz", None, None),
    )
    return jax.shard_map(
        local, mesh=mesh, in_specs=in_specs, out_specs=(field,) * 3, check_vma=False
    )
```

```python
import functools

import jax
import jax.numpy as jnp
import numpy as np
from jax import lax
from jax.experimental import pallas as pl
from jax.experimental.pallas import tpu as pltpu
from jax.sharding import PartitionSpec as P

STAR = (-205.0 / 72.0, 8.0 / 5.0, -1.0 / 5.0, 8.0 / 315.0, -1.0 / 560.0)
CX, CY, CZ, STEPS, RECS = 16, 32, 128, 4, 128
ROWS = CX * CY
UNROLL = 16
AXES = ("gx", "gy", "gz")
MESH = pl.DeviceIdType.MESH
F32, BF16 = jnp.float32, jnp.bfloat16


def split_np(table):
    high = table.astype(np.float32).astype(jnp.bfloat16)
    low = (table - high.astype(np.float64)).astype(np.float32).astype(jnp.bfloat16)
    return high, low


def tables():
    freq, place = np.arange(4)[:, None], np.arange(4)[None, :]
    dct = np.where(freq == 0, 0.5, np.sqrt(0.5)) * np.cos(np.pi * (2 * place + 1) * freq / 8)
    along_z = np.kron(np.eye(CZ // 4), dct)
    along_xy = np.kron(dct.T, np.kron(np.eye(CY // 4), dct.T))
    gap = np.abs(np.arange(CZ)[:, None] - np.arange(CZ)[None, :])
    taps = np.select([gap == k for k in range(1, 5)], STAR[1:], 0.0)
    taps_hl = np.concatenate(split_np(taps), axis=1)
    z_hl = np.concatenate(split_np(along_z), axis=1)
    decode_xy = np.concatenate(split_np(along_xy), axis=1)
    spread_z = np.kron(np.eye(CZ // 4), np.ones((1, 4)))
    spread_y = np.kron(np.eye(STEPS * CX // 4), np.kron(np.eye(CY // 4), np.ones((4, 1))))
    spread = np.concatenate([spread_z, spread_y]).astype(jnp.bfloat16)
    spread = np.pad(spread, ((0, 0), (0, CZ)))
    return np.concatenate([taps_hl, taps_hl, z_hl, z_hl, decode_xy, spread])


def split(value):
    high = value.astype(BF16)
    low = (value - high.astype(F32)).astype(BF16)
    return high, low


def dot(a, b):
    return lax.dot_general(a, b, (((1,), (0,)), ((), ())), preferred_element_type=F32)


def halves(value):
    return value[:, :CZ] + value[:, CZ:]


def kernel(
    coef, keep, cour, damp, nxt, now, cell, data, ops,
    grad_o, last_o, before_o,
    F, cin, kin, edge_v, trio, cell_v, data_v, ops_v,
    wa, wb, we, inj, thr, Z, XH, YP, YH, CP, XC, XP, XM, XL, XT, ZP, ZH,
    load_sem, send_sem, step_sem, row_sem, forward_sem, edge_sem,
):
    me = [lax.axis_index(axis) for axis in AXES]
    size = [lax.axis_size(axis) for axis in AXES]
    has = [(me[d] > 0, me[d] < size[d] - 1) for d in range(3)]
    other = [({AXES[d]: me[d] - 1}, {AXES[d]: me[d] + 1}) for d in range(3)]

    barrier = pltpu.get_barrier_semaphore()
    for d in (1, 0, 2):
        for side in range(2):
            @pl.when(has[d][side])
            def _():
                pl.semaphore_signal(
                    barrier, inc=1, device_id=other[d][side], device_id_type=MESH
                )

    def load(n, src, dst):
        return pltpu.make_async_copy(src, dst, load_sem.at[n])

    edges = [load(n, now.at[:, pl.ds(24 * n, 8)], edge_v.at[n]) for n in range(2)]
    first = load(2, now, F.at[0, pl.ds(4, CX), pl.ds(8, CY)])
    tables_in = [load(3, ops, ops_v), load(4, keep, kin), load(5, coef, cin)]
    points_in = [load(7, cell, cell_v), load(8, data, data_v)]
    fields_in = [load(6, src, trio.at[n]) for n, src in enumerate((cour, damp, nxt))]
    cour_v, damp_v, next_v = (trio.at[n] for n in range(3))
    for copy in edges + [first]:
        copy.start()

    def clear(f, carry):
        F[f, 0:4] = jnp.zeros((4, 48, CZ), F32)
        F[f, 20:24] = jnp.zeros((4, 48, CZ), F32)
        F[f, 4:20, 0:8] = jnp.zeros((CX, 8, CZ), F32)
        F[f, 4:20, 40:48] = jnp.zeros((CX, 8, CZ), F32)
        for side in range(2):
            YH[f, side, 0:8] = jnp.zeros((8, CZ), F32)
            YH[f, side, 72:80] = jnp.zeros((8, CZ), F32)

            @pl.when(jnp.logical_not(has[0][side]))
            def _():
                XH[f, side] = jnp.zeros((4, CY, CZ), F32)

            @pl.when(jnp.logical_not(has[1][side]))
            def _():
                YH[f, side, 8:72] = jnp.zeros((64, CZ), F32)

            @pl.when(jnp.logical_not(has[2][side]))
            def _():
                ZH[f, side] = jnp.zeros((16, CZ), F32)

        return carry

    lax.fori_loop(0, 8, clear, 0)
    for side in range(2):
        XT[side] = jnp.zeros((4, 16, CZ), F32)
        for f in range(1, STEPS):
            for row in (0, 24):
                XH[f, side, :, row : row + 8] = jnp.zeros((4, 8, CZ), F32)
        for f in range(STEPS):
            CP[f, side, 0:8] = jnp.zeros((8, CZ), F32)
            CP[f, side, 72:80] = jnp.zeros((8, CZ), F32)

        @pl.when(jnp.logical_not(has[1][side]))
        def _():
            YH[8, side, 8:72] = jnp.zeros((64, CZ), F32)

    lane = lax.broadcasted_iota(jnp.int32, (8, CZ), 1)
    sub = lax.broadcasted_iota(jnp.int32, (8, CZ), 0)
    near_low = [None] + [jnp.where(sub < k, STAR[k], 0.0).astype(F32) for k in range(1, 5)]
    across = [
        [None] + [jnp.where(sub % 4 >= 4 - k, STAR[k], 0.0).astype(F32) for k in range(1, 5)],
        [None] + [jnp.where(sub % 4 < k, STAR[k], 0.0).astype(F32) for k in range(1, 5)],
    ]
    near_high = [None] + [jnp.where(sub >= 8 - k, STAR[k], 0.0).astype(F32) for k in range(1, 5)]

    def faces(f, d, side, some=slice(None)):
        if d == 0 and 0 < f < STEPS:
            inner, there = pl.ds(8, 16), 1 - side
            pairs = [(F.at[f, pl.ds(4 + 12 * side, 4), pl.ds(16, 16)], XH.at[f, there, :, inner])]
            pairs += [(XP.at[f - 1, side, t], XM.at[f - 1, there, t]) for t in range(2)]
            row = pl.ds(8 + 48 * side, 16)
            pairs += [(CP.at[f, t, row], XL.at[f - 1, there, t]) for t in range(2)]
        elif d == 0:
            start = 4 if side == 0 else CX
            pairs = [(F.at[f, pl.ds(start, 4), pl.ds(8, CY)], XH.at[f, 1 - side])]
        elif d == 1:
            pairs = [
                (YP.at[f, side, pl.ds(row, 16)], YH.at[f, 1 - side, pl.ds(8 + row, 16)])
                for row in range(0, 64, 16)
            ]
        else:
            pairs = [(ZP.at[f, side], ZH.at[f, 1 - side])]
        return [
            copy_to(f, d, side, src, dst, n) for n, (src, dst) in list(enumerate(pairs))[some]
        ]

    def copy_to(f, d, side, src, dst, n=0):
        if d == 0 and n > 2:
            landed = edge_sem.at[f % 2, 1 - side]
        elif d == 1:
            landed = row_sem.at[f, 1 - side]
        elif f < STEPS:
            landed = step_sem.at[f % 2, d // 2, 1 - side]
        else:
            landed = forward_sem.at[f - STEPS, d // 2, 1 - side]
        return pltpu.make_async_remote_copy(
            src_ref=src,
            dst_ref=dst,
            send_sem=send_sem.at[d, side],
            recv_sem=landed,
            device_id=other[d][side],
            device_id_type=MESH,
        )

    def whole(f, d, side, n=0):
        from_ref, to_ref = ((XH, XH), (YP, YP), (ZP, ZH))[d]
        src, dst = from_ref.at[f, side], to_ref.at[f, 1 - side]
        if d == 0 and 0 < f < STEPS:
            src, dst = (ref.at[:, pl.ds(0, 8 if n else 24)] for ref in (src, dst))
        return copy_to(f, d, side, src, dst, n)

    def each_side(d, act):
        for side in range(2):
            @pl.when(has[d][side])
            def _():
                act(side)

    def send(f, d, some=slice(None)):
        each_side(d, lambda side: [copy.start() for copy in faces(f, d, side, some)])

    def arrive(f, d, n=0):
        each_side(d, lambda side: whole(f, d, 1 - side, n).wait_recv())

    def drain(d):
        every = (XH, YP, ZP)[d]
        each_side(
            d, lambda side: copy_to(0, d, side, every.at[:, side], every.at[:, side]).wait_send()
        )

    def pack_rows(f):
        def pack_y(p, carry):
            for side, row in ((0, 8), (1, 36)):
                two = [F[f, 4 + 2 * p + q, row : row + 4, :] for q in range(2)]
                YP[f, side, pl.ds(pl.multiple_of(8 * p, 8), 8), :] = jnp.concatenate(two, axis=0)
            return carry

        lax.fori_loop(0, 8, pack_y, 0, unroll=True)

    def pack_lanes(f):
        def pack_z(q, kept):
            kept = list(kept)
            for tile in range(4):
                i = 4 * q + tile
                here = lane // 4 == i
                for half in range(2):
                    value = F[f, 4 + 8 * half + q, 8 + 8 * tile : 16 + 8 * tile, :]
                    low = pltpu.roll(value, 4 * i, 1)
                    high = pltpu.roll(value, (4 * i + 4) % CZ, 1)
                    kept[half] = jnp.where(here, low, kept[half])
                    kept[2 + half] = jnp.where(here, high, kept[2 + half])
            return tuple(kept)

        zero = jnp.zeros((8, CZ), F32)
        kept = lax.fori_loop(0, 8, pack_z, (zero,) * 4, unroll=True)
        for side in range(2):
            for half in range(2):
                ZP[f, side, 8 * half : 8 * half + 8, :] = kept[2 * side + half]

    def own_z(f):
        value = F[f, 4:20, 8:40, :].reshape(ROWS, CZ)
        return halves(dot(jnp.concatenate(split(value), axis=1), ops_v[0:256]))

    def far_z(f):
        member = lane % 4
        out = []
        for half in range(2):
            low = ZH[f, 0, 8 * half : 8 * half + 8, :]
            high = ZH[f, 1, 8 * half : 8 * half + 8, :]
            low_sum = STAR[4] * low
            high_sum = STAR[4] * high
            for k in range(1, 4):
                gap = 4 - k
                low_sum = low_sum + jnp.where(
                    member < k, STAR[k] * pltpu.roll(low, CZ - gap, 1), 0.0
                )
                high_sum = high_sum + jnp.where(
                    member >= gap, STAR[k] * pltpu.roll(high, gap, 1), 0.0
                )
            out.append((low_sum, high_sum))
        return out

    def add_z(f, target, scale):
        packed = far_z(f)
        for v in range(64):
            half, i = divmod(v, 32)
            low = pltpu.roll(packed[half][0], (CZ - 4 * i) % CZ, 1)
            high = pltpu.roll(packed[half][1], (252 - 4 * i) % CZ, 1)
            value = jnp.where(lane < 4, low, jnp.where(lane >= CZ - 4, high, 0.0))
            x, row = v // 4, 8 * (v % 4)
            at = (x, slice(row, row + 8))
            target[at] = target[at] + scale(*at) * value

    def add_x(f, target, scale, parts=((0, CY),)):
        for start, stop in parts:
            rows = slice(start, stop)
            for i in range(4):
                low = sum(STAR[k] * XH[f, 0, 4 + i - k, rows] for k in range(i + 1, 5))
                high = sum(STAR[4 + m - i] * XH[f, 1, m, rows] for m in range(i + 1))
                target[i, rows] = target[i, rows] + scale(i, rows) * low
                target[12 + i, rows] = target[12 + i, rows] + scale(12 + i, rows) * high

    def near_y(f, x):
        at = 4 * x
        low = sum(near_low[k] * YH[f, 0, 12 + at - k : 20 + at - k] for k in range(1, 5))
        high = sum(near_high[k] * YH[f, 1, at + k : at + k + 8] for k in range(1, 5))
        return low, high

    def own_star(f, x):
        total = (3.0 * STAR[0]) * F[f, 4 + x, 8:40, :] + Z[x]
        for k in range(1, 5):
            pairs = F[f, 4 + x + k, 8:40, :] + F[f, 4 + x - k, 8:40, :]
            pairs = pairs + F[f, 4 + x, 8 + k : 40 + k, :] + F[f, 4 + x, 8 - k : 40 - k, :]
            total = total + STAR[k] * pairs
        return total

    def target_of(s):
        return last_o if s == STEPS - 1 else F.at[s + 1, pl.ds(4, CX), pl.ds(8, CY)]

    def adjoint_own(s):
        Z[...] = own_z(s).reshape(CX, CY, CZ)
        target = target_of(s)

        def step(x, carry):
            later = next_v[x] if s == 0 else F[s - 1, 4 + x, 8:40, :]
            current = F[s, 4 + x, 8:40, :]
            target[x] = wa[x] * current - wb[x] * later + we[x] * own_star(s, x) + inj[s, x]
            if s == STEPS - 1:
                before_o[x] = current
            return carry

        lax.fori_loop(0, CX, step, 0, unroll=UNROLL)

    def send_partial(f, pieces):
        target = target_of(f - 1)
        for n in pieces:
            for p in (2 * n, 2 * n + 1):
                for side, row in ((0, 0), (1, 28)):
                    two = [target[2 * p + q, row : row + 4, :] for q in range(2)]
                    YP[f, side, 8 * p : 8 * p + 8] = jnp.concatenate(two, axis=0)
        for n in pieces:
            send(f, 1, slice(n, n + 1))

    def step_scale(*at):
        return we[at]

    def adjoint_near(s):
        target = target_of(s)
        sends = s < STEPS - 1
        arrive(s, 2)
        add_z(s, target, step_scale)
        if sends:
            send_partial(s + 1, (1, 2))
        arrive(s, 0)
        if s > 0:
            each_side(0, lambda side: place(XM.at[s - 1, side], XH.at[s, side], ((0, 4), (1, 24))))
        add_x(s, target, step_scale)
        if sends:
            send(s + 1, 0, slice(0, 1))
            for side in range(2):
                for t, row in ((0, 4), (1, 24)):
                    for p in range(2):
                        two = [target[12 * side + 2 * p + q, row : row + 4, :] for q in range(2)]
                        XP[s, side, t, 8 * p : 8 * p + 8] = jnp.concatenate(two, axis=0)
            send(s + 1, 0, slice(1, 3))
        if s > 0:
            arrive(s, 0, 3)
            each_side(0, lambda side: place(XL.at[s - 1, side], XT.at[side], ((0, 0), (1, 12))))
            for t, rows in ((0, slice(0, 8)), (1, slice(24, 32))):
                own = slice(8 * t, 8 * t + 8)
                for i in range(4):
                    low = sum(STAR[k] * XT[0, 4 + i - k, own] for k in range(i + 1, 5))
                    high = sum(STAR[4 + m - i] * XT[1, m, own] for m in range(i + 1))
                    target[i, rows] = target[i, rows] + we[i, rows] * low
                    target[12 + i, rows] = target[12 + i, rows] + we[12 + i, rows] * high
        if sends:
            send_partial(s + 1, (0, 3))

    def place(packed, slabs, spots):
        for t, row in spots:
            for i in range(4):
                slabs[i, row : row + 4] = packed[t, 4 * i : 4 * i + 4]

    def cross(f):
        for p in range(8):
            at = 8 + 8 * p
            for side in range(2):
                total = 0.0
                for k in range(1, 5):
                    move = k - 4 if side == 0 else 4 - k
                    part = CP[f - 1, side, at + move : at + move + 8]
                    total = total + across[side][k] * part
                XC[side, 8 * p : 8 * p + 8] = YH[8, side, at : at + 8] * total

    def adjoint_rows(s):
        target = target_of(s)
        sends = s < STEPS - 1
        arrive(s, 1)
        if s > 0:
            for side in range(2):
                YH[s, side, 8:72] = YH[s, side, 8:72] + XC[side]
        for p in range(8):
            lows, highs = [], []
            for x in (2 * p, 2 * p + 1):
                low, high = near_y(s, x)
                low = target[x, 0:8] + we[x, 0:8] * low
                high = target[x, 24:32] + we[x, 24:32] * high
                lows.append(low[0:4])
                highs.append(high[4:8])
                target[x, 0:8] = low
                target[x, 24:32] = high
            if sends:
                CP[s + 1, 0, 8 + 8 * p : 16 + 8 * p] = jnp.concatenate(lows, axis=0)
                CP[s + 1, 1, 8 + 8 * p : 16 + 8 * p] = jnp.concatenate(highs, axis=0)
        if sends:
            send(s + 1, 0, slice(3, 5))
            pack_lanes(s + 1)
            send(s + 1, 2)

    def decode(s):
        level = (
            lax.broadcasted_iota(jnp.int32, (CY, CZ), 0) % 4
            + lax.broadcasted_iota(jnp.int32, (CY, CZ), 1) % 4
        ).astype(F32)
        masked = [
            jnp.where(level + float(x % 4) < thr[s, x // 4], cin[s, x], 0.0) for x in range(CX)
        ]
        value = jnp.concatenate(masked, axis=0)
        along_z = halves(dot(jnp.concatenate(split(value), axis=1), ops_v[256:512]))
        for g in range(CX // 4):
            both = jnp.concatenate(split(along_z[CZ * g : CZ * g + CZ]), axis=1)
            out = halves(dot(ops_v[512:640], jnp.concatenate([both, both], axis=0)))
            F[4 + s, 4 + 4 * g : 8 + 4 * g, 8:40, :] = out.reshape(4, CY, CZ)

    def gradient_own(s):
        Z[...] = own_z(4 + s).reshape(CX, CY, CZ)

        def step(x, carry):
            value = cour_v[x] * F[s, 4 + x, 8:40, :] * own_star(4 + s, x)
            grad_o[x] = value if s == 0 else grad_o[x] + value
            return carry

        lax.fori_loop(0, CX, step, 0, unroll=UNROLL)

    def gradient_far(s):
        f = 4 + s
        current = F.at[s, pl.ds(4, CX), pl.ds(8, CY)]

        def scale(*at):
            return cour_v[at] * current[at]

        arrive(f, 2)
        add_z(f, grad_o, scale)
        arrive(f, 0)
        add_x(f, grad_o, scale)
        arrive(f, 1)
        for x in range(CX):
            low, high = near_y(f, x)
            top, end = slice(0, 8), slice(24, 32)
            grad_o[x, top] = grad_o[x, top] + scale(x, top) * low
            grad_o[x, end] = grad_o[x, end] + scale(x, end) * high

    def prepare(s):
        decode(s)
        pack_rows(4 + s)
        pack_lanes(4 + s)

    def post(s, dims=(1, 0, 2)):
        for d in dims:
            send(4 + s, d)

    for copy in edges:
        copy.wait()
    for copy in tables_in + fields_in + points_in:
        copy.start()
    for p in range(8):
        for side in range(2):
            two = [edge_v[side, 2 * p + q, 4 * side : 4 * side + 4, :] for q in range(2)]
            rows = jnp.concatenate(two, axis=0)
            YP[0, side, 8 * p : 8 * p + 8, :] = rows
            CP[0, side, 8 + 8 * p : 16 + 8 * p, :] = rows
    peers = sum(there.astype(jnp.int32) for pair in has for there in pair)
    pl.semaphore_wait(barrier, peers)
    send(0, 1)
    first.wait()
    send(0, 0)
    pack_lanes(0)
    send(0, 2)

    load(6, trio, trio).wait()
    for copy in points_in:
        copy.wait()

    def weights(x, carry):
        over = 1.0 / (1.0 + damp_v[x])
        wa[x] = 2.0 * over
        wb[x] = (1.0 - damp_v[x]) * over
        we[x] = cour_v[x] * over
        return carry

    lax.fori_loop(0, CX, weights, 0, unroll=2)

    for p in range(8):
        for side in range(2):
            row = 28 * side
            two = [we[2 * p + q, row : row + 4, :] for q in range(2)]
            YP[8, side, 8 * p : 8 * p + 8] = jnp.concatenate(two, axis=0)
    send(8, 1)

    row = lax.broadcasted_iota(jnp.int32, (ROWS, RECS), 0)
    rows_hot = jnp.where(row == cell_v[...] // CZ, 1.0, 0.0).astype(BF16)
    rows_hot = jnp.concatenate([rows_hot, rows_hot], axis=1)
    at_lane = lax.broadcasted_iota(jnp.int32, (CZ, RECS), 0) == cell_v[...] % CZ
    for s in range(STEPS):
        lanes_hot = jnp.where(at_lane, data_v[s : s + 1, :], 0.0)
        lanes_hot = jnp.concatenate(split(lanes_hot), axis=1)
        spread = lax.dot_general(
            rows_hot, lanes_hot, (((1,), (1,)), ((), ())), preferred_element_type=F32
        )
        inj[s] = spread.reshape(CX, CY, CZ) * (0.5 * wa[...])

    for copy in tables_in:
        copy.wait()
    levels = kin[...].reshape(STEPS * (CX // 4) * (CY // 4), CZ // 4).astype(F32).astype(BF16)
    wide = dot(levels, ops_v[640:672, 0:CZ]).astype(BF16)
    thr[...] = jnp.concatenate([dot(ops_v[672 + 256 * h : 928 + 256 * h, 0:CZ], wide) for h in range(2)]).reshape(STEPS, CX // 4, CY, CZ)

    prepare(0)
    post(0, (0, 2))
    adjoint_own(0)
    prepare(1)
    adjoint_near(0)
    post(0, (1,))
    adjoint_rows(0)
    post(1)
    arrive(8, 1)

    adjoint_own(1)
    cross(1)
    prepare(2)
    gradient_own(0)
    adjoint_near(1)
    adjoint_rows(1)
    post(2)

    adjoint_own(2)
    cross(2)
    prepare(3)
    post(3)
    gradient_own(1)
    gradient_far(0)
    adjoint_near(2)
    adjoint_rows(2)

    adjoint_own(3)
    cross(3)
    gradient_own(2)
    gradient_own(3)
    gradient_far(1)
    gradient_far(2)
    adjoint_near(3)
    gradient_far(3)
    adjoint_rows(3)
    for d in range(3):
        drain(d)


def put_out(grad_v, last_v, before_v, grad_o, last_o, before_o, sem):
    pairs = ((grad_v, grad_o), (last_v, last_o), (before_v, before_o))
    copies = [pltpu.make_async_copy(v, o, sem.at[n]) for n, (v, o) in enumerate(pairs)]
    for copy in copies:
        copy.start()
    for copy in copies:
        copy.wait()


def local(coef, keep, courant, damp, adj_next, adj_now, rec_cell, rec_data):
    shape = (CX, CY, CZ)
    block = jax.ShapeDtypeStruct(shape, F32)
    ops = tables()
    vmem = pltpu.VMEM
    scratch = [
        vmem((8, 24, 48, CZ), F32),
        vmem((STEPS,) + shape, F32),
        vmem((STEPS, CX // 4, CY // 4, CZ // 4), jnp.int32),
        vmem((2, CX, 8, CZ), F32), vmem((3,) + shape, F32),
        vmem((1, RECS), jnp.int32), vmem((STEPS, RECS), F32), vmem(ops.shape, BF16),
        vmem(shape, F32), vmem(shape, F32), vmem(shape, F32),
        vmem((STEPS,) + shape, F32),
        vmem((STEPS, CX // 4, CY, CZ), F32),
        vmem(shape, F32),
        vmem((8, 2, 4, CY, CZ), F32),
        vmem((9, 2, 64, CZ), F32), vmem((9, 2, 80, CZ), F32),
        vmem((STEPS, 2, 80, CZ), F32), vmem((2, 64, CZ), F32),
        vmem((STEPS - 1, 2, 2, 16, CZ), F32), vmem((STEPS - 1, 2, 2, 16, CZ), F32),
        vmem((STEPS - 1, 2, 2, 16, CZ), F32), vmem((2, 4, 16, CZ), F32),
        vmem((8, 2, 16, CZ), F32), vmem((8, 2, 16, CZ), F32),
        pltpu.SemaphoreType.DMA((9,)),
        pltpu.SemaphoreType.DMA((3, 2)), pltpu.SemaphoreType.DMA((2, 2, 2)),
        pltpu.SemaphoreType.DMA((9, 2)), pltpu.SemaphoreType.DMA((STEPS, 2, 2)),
        pltpu.SemaphoreType.DMA((2, 2)),
    ]
    vmem_spec = pl.BlockSpec(memory_space=pltpu.VMEM)
    hbm_spec = pl.BlockSpec(memory_space=pltpu.HBM)
    results = pl.pallas_call(
        kernel,
        out_shape=(vmem(shape, F32),) * 3,
        in_specs=[hbm_spec] * 9,
        out_specs=(vmem_spec,) * 3,
        scratch_shapes=scratch,
        compiler_params=pltpu.CompilerParams(
            collective_id=0, has_side_effects=True, vmem_limit_bytes=67043328 - 3 * 4 * CX * CY * CZ
        ),
        name="adjoint_window",
    )(
        coef, keep, courant, damp, adj_next, adj_now,
        rec_cell.reshape(1, RECS), rec_data.reshape(STEPS, RECS),
        jnp.asarray(ops),
    )
    return pl.pallas_call(
        put_out,
        out_shape=(block,) * 3,
        in_specs=[pl.BlockSpec(memory_space=pl.ANY)] * 3,
        out_specs=(hbm_spec,) * 3,
        scratch_shapes=[pltpu.SemaphoreType.DMA((3,))],
        compiler_params=pltpu.CompilerParams(vmem_limit_bytes=1024 * 1024),
        name="put_out",
    )(*results)


def solution(mesh):
    field = P("gx", "gy", "gz")
    in_specs = (
        P(None, "gx", "gy", "gz"), P(None, "gx", "gy", "gz"),
        field, field, field, field,
        P("gx", "gy", "gz", None), P("gx", "gy", "gz", None, None),
    )
    return jax.shard_map(
        local, mesh=mesh, in_specs=in_specs, out_specs=(field,) * 3, check_vma=False
    )
```
